128 devices in a mesh: fsdp: 8 (over z_lo, x), tp: 16 (over y, z_hi, core).
Axes of the slice: x: 4, y: 4, z: 4 (z_hi: 2, z_lo: 2; z = z_hi * 2 + z_lo), core: 2. Of those that a mesh axis runs over, the one named last changes fastest.
Arguments:
- ref_gate: bfloat16 [6144, 11008], P('fsdp', 'tp'), may hold values from -6 to 6
- ref_up: bfloat16 [6144, 11008], P('fsdp', 'tp'), may hold values from -6 to 6
- ref_residual: bfloat16 [6144, 4096], P('fsdp', 'tp'), may hold values from -6 to 6
- ref_modality: int32 [6144], P('fsdp'), may hold values 0 or 1
- ref_down_text: bfloat16 [4096, 11008], P('fsdp', 'tp'), may hold values from -0.0546875 to 0.0546875
- ref_down_image: bfloat16 [4096, 11008], P('fsdp', 'tp'), may hold values from -0.0546875 to 0.0546875
- pol_gate: bfloat16 [6144, 11008], P('fsdp', 'tp'), may hold values from -6 to 6
- pol_up: bfloat16 [6144, 11008], P('fsdp', 'tp'), may hold values from -6 to 6
- pol_modality: int32 [6144], P('fsdp'), may hold values 0 or 1
- pol_segment: int32 [6144], P('fsdp'), may hold values from 0 to 11, never falling along the last dimension, each value on 1 to 768 neighbouring positions
- pair_margin: float32 [6], replicated, may hold values from -30 to 30
- token_cotangent: bfloat16 [6144, 4096], P('fsdp', 'tp'), may hold values from -24 to 24
- pol_down_text: bfloat16 [4096, 11008], P('fsdp', 'tp'), may hold values from -0.0546875 to 0.0546875
- pol_down_image: bfloat16 [4096, 11008], P('fsdp', 'tp'), may hold values from -0.0546875 to 0.0546875
Outputs:
- ref_out: bfloat16 [6144, 4096], P('fsdp', 'tp')
- grad_gate: bfloat16 [6144, 11008], P('fsdp', 'tp')
- grad_up: bfloat16 [6144, 11008], P('fsdp', 'tp')
- grad_down_text: float32 [4096, 11008], P('fsdp', 'tp')
- grad_down_image: float32 [4096, 11008], P('fsdp', 'tp')
The draws below stay inside these ranges and needn't reach their ends.
Inputs may be any that keep to these rules, and one draw needn't show every extreme that they name: `ref_modality`: 0 marks a text token, 1 an image token. `pol_modality`: 0 marks a text token, 1 an image token. `pol_segment`: response numbers never fall along the tokens; responses 2p and 2p + 1 are the chosen and the rejected response of pair p; every response has at least one token.
All inputs are finite; a program needn't handle non-finite values. No bound on the sum of `ref_modality` or of `pol_modality` on one device may be relied on, other than what follows from the above.
Results may differ from the reference program's by a relative error of at most 0.015.
Values may be sent and summed in bfloat16 or wider, within the bound.
A program may use at most 128 MiB of HBM per device.

```python
import math
import jax
import jax.numpy as jnp
import numpy as np
from jax import lax

D = 4096
FF = 11008
SEQ = 512
TOKENS = 6144
PAIRS = 6
N_FSDP = 8
N_TP = 16


def plant(entries, rng, smallest, top_value):
    longest = entries.shape.index(max(entries.shape))
    spots = []
    for shift in (0, 1):
        where = [jax.random.randint(jax.random.fold_in(rng, axis), (), 0, length) for axis, length in enumerate(entries.shape)]
        where[longest] = (where[longest] + shift) % entries.shape[longest]
        spots.append(tuple(where))
    return entries.at[spots[0]].set(smallest).at[spots[1]].set(top_value)


def block_levels(own_key, dims, pieces, least, largest):
    def one(position, shards_of):
        steps = jax.random.uniform(jax.random.fold_in(jax.random.fold_in(own_key, 6), position), (shards_of,), jnp.float32, least / len(pieces), largest / len(pieces))
        return jnp.repeat(jnp.exp(steps), dims[position] // shards_of).reshape((-1,) + (1,) * (len(dims) - position - 1))

    factor_of = one(*pieces[0])
    for cut in pieces[1:]:
        factor_of = factor_of * one(*cut)
    return factor_of


def profile(number_of, total, bound, slope):
    weights = [(1 << 20) // math.isqrt(standing ** slope) + 1 for standing in range(2, number_of + 1)]
    spare, counts = total - bound - (number_of - 1), [1] * (number_of - 1)
    while spare > 0:
        movable = [i for i in range(number_of - 1) if counts[i] < bound]
        whole, left = sum([weights[i] for i in movable]), spare
        for i in movable:
            extra = min(bound - counts[i], max(1, left * weights[i] // whole), spare)
            counts[i] = counts[i] + extra
            spare = spare - extra
    return np.array([bound] + counts)


def ragged_sizes(own_key, amount, total, bound, lean):
    if amount == 2:
        one = jax.random.randint(own_key, (), max(1, total - bound), min(bound, total - 1) + 1)
        return jnp.stack([one, total - one])
    lengths = jnp.asarray(profile(amount, total, bound, lean), jnp.int32)
    twos = (amount - 1) // 2
    source_of, receiver = lengths[1:1 + 2 * twos:2], lengths[2:2 + 2 * twos:2]
    margin = jnp.minimum(source_of - 1, bound - receiver)
    shifted = jax.random.randint(jax.random.fold_in(own_key, 1), (twos,), 0, 1 << 20) % (margin + 1)
    lengths = lengths.at[1:1 + 2 * twos:2].set(source_of - shifted).at[2:2 + 2 * twos:2].set(receiver + shifted)
    return lengths[jax.random.permutation(jax.random.fold_in(own_key, 2), amount)]


def normal_values(rng, dims, deviation, limit, pieces=(), held_as=jnp.bfloat16):
    factor_of = block_levels(rng, dims, pieces, -0.22, 0.18) if pieces else 1.0
    result = jax.random.normal(rng, dims, jnp.float32) * deviation * factor_of
    return jnp.minimum(jnp.maximum(result, -limit), limit).astype(held_as)


def setup_inputs(seed: int = 0) -> dict:
    seeds = jax.random.split(jax.random.key(seed), 15)
    ref_gate = normal_values(seeds[0], (TOKENS, FF), 1.0, 6.0, ((0, 8), (1, 16)))
    ref_up = normal_values(seeds[1], (TOKENS, FF), 1.0, 6.0, ((0, 8), (1, 16)))
    ref_residual = normal_values(seeds[2], (TOKENS, D), 1.0, 6.0, ((0, 8), (1, 16)))
    ref_modality = plant((jax.random.randint(seeds[3], (TOKENS,), 0, 5) < 2).astype(jnp.int32), jax.random.fold_in(seeds[3], 1), 0, 1)
    ref_down_text = normal_values(seeds[4], (D, FF), FF ** -0.5, 0.0546875, ((0, 8), (1, 16)))
    ref_down_image = normal_values(seeds[5], (D, FF), FF ** -0.5, 0.0546875, ((0, 8), (1, 16)))
    pol_gate = normal_values(seeds[6], (TOKENS, FF), 1.0, 6.0, ((0, 8), (1, 16)))
    pol_up = normal_values(seeds[7], (TOKENS, FF), 1.0, 6.0, ((0, 8), (1, 16)))
    pol_modality = plant((jax.random.randint(seeds[8], (TOKENS,), 0, 5) < 2).astype(jnp.int32), jax.random.fold_in(seeds[8], 1), 0, 1)
    pol_segment = jnp.searchsorted(jnp.cumsum(ragged_sizes(seeds[9], 2 * PAIRS, TOKENS, SEQ + SEQ // 2, 0)), jnp.arange(TOKENS), side="right").astype(jnp.int32)
    pair_margin = jnp.clip(jax.random.uniform(seeds[10], (PAIRS,), jnp.float32, -30.0, 30.0), -30.0, 30.0)
    token_cotangent = normal_values(seeds[11], (TOKENS, D), 4.0, 24.0, ((0, 8), (1, 16)))
    pol_down_text = normal_values(seeds[12], (D, FF), FF ** -0.5, 0.0546875, ((0, 8), (1, 16)))
    pol_down_image = normal_values(seeds[13], (D, FF), FF ** -0.5, 0.0546875, ((0, 8), (1, 16)))
    return {"ref_gate": ref_gate, "ref_up": ref_up, "ref_residual": ref_residual, "ref_modality": ref_modality, "ref_down_text": ref_down_text, "ref_down_image": ref_down_image, "pol_gate": pol_gate, "pol_up": pol_up, "pol_modality": pol_modality, "pol_segment": pol_segment, "pair_margin": pair_margin, "token_cotangent": token_cotangent, "pol_down_text": pol_down_text, "pol_down_image": pol_down_image}


dpo_beta = 0.1


def split_hidden(gate, up, modality):
    gate_f = gate.astype(jnp.float32)
    up_f = up.astype(jnp.float32)
    sig = jax.nn.sigmoid(gate_f)
    act = gate_f * sig
    hidden = (act * up_f).astype(jnp.bfloat16)
    image = (modality == 1)[:, None]
    zero = jnp.zeros_like(hidden)
    return jnp.where(image, zero, hidden), jnp.where(image, hidden, zero), gate_f, up_f, sig, act


def reference(ref_gate, ref_up, ref_residual, ref_modality, ref_down_text, ref_down_image, pol_gate, pol_up, pol_modality, pol_segment, pair_margin, token_cotangent, pol_down_text, pol_down_image):
    ref_text, ref_image, _, _, _, _ = split_hidden(ref_gate, ref_up, ref_modality)
    block_width = FF // N_TP
    contract = (((1,), (1,)), ((), ()))

    def ref_block(index, total):
        start = (index * block_width).astype(jnp.int32)
        left_text = lax.dynamic_slice_in_dim(ref_text, start, block_width, 1)
        left_image = lax.dynamic_slice_in_dim(ref_image, start, block_width, 1)
        right_text = lax.dynamic_slice_in_dim(ref_down_text, start, block_width, 1)
        right_image = lax.dynamic_slice_in_dim(ref_down_image, start, block_width, 1)
        part = lax.dot_general(left_text, right_text, contract, preferred_element_type=jnp.float32)
        part = part + lax.dot_general(left_image, right_image, contract, preferred_element_type=jnp.float32)
        rounded = lax.optimization_barrier(part.astype(jnp.bfloat16))
        return total + rounded.astype(jnp.float32)

    summed = lax.fori_loop(0, N_TP, ref_block, jnp.zeros((TOKENS, D), jnp.float32))
    ref_out = (summed + ref_residual.astype(jnp.float32)).astype(jnp.bfloat16)

    pol_text, pol_image, gate_f, up_f, sig, act = split_hidden(pol_gate, pol_up, pol_modality)
    seg_ids = jnp.arange(2 * PAIRS, dtype=jnp.int32)
    pair_weight = dpo_beta * jax.nn.sigmoid(-dpo_beta * pair_margin)
    table = jnp.repeat(pair_weight, 2) * jnp.where(seg_ids % 2 == 0, -1.0, 1.0).astype(jnp.float32)
    coef = jnp.sum(jnp.where(pol_segment[:, None] == seg_ids[None, :], table[None, :], jnp.float32(0.0)), axis=1)
    cot = (coef[:, None] * token_cotangent.astype(jnp.float32)).astype(jnp.bfloat16)
    image_p = (pol_modality == 1)[:, None]
    zero_cot = jnp.zeros_like(cot)
    cot_text = jnp.where(image_p, zero_cot, cot)
    cot_image = jnp.where(image_p, cot, zero_cot)
    d_hidden = jnp.dot(cot_text, pol_down_text, preferred_element_type=jnp.float32)
    d_hidden = d_hidden + jnp.dot(cot_image, pol_down_image, preferred_element_type=jnp.float32)
    grad_gate = (d_hidden * up_f * sig * (1.0 + gate_f * (1.0 - sig))).astype(jnp.bfloat16)
    grad_up = (d_hidden * act).astype(jnp.bfloat16)

    rows_block = TOKENS // N_FSDP
    over_rows = (((0,), (0,)), ((), ()))

    def grad_block(index, totals):
        start = (index * rows_block).astype(jnp.int32)
        y_text = lax.dynamic_slice_in_dim(cot_text, start, rows_block, 0)
        y_image = lax.dynamic_slice_in_dim(cot_image, start, rows_block, 0)
        h_text = lax.dynamic_slice_in_dim(pol_text, start, rows_block, 0)
        h_image = lax.dynamic_slice_in_dim(pol_image, start, rows_block, 0)
        term_text = lax.dot_general(y_text, h_text, over_rows, preferred_element_type=jnp.float32)
        term_image = lax.dot_general(y_image, h_image, over_rows, preferred_element_type=jnp.float32)
        term_text = lax.optimization_barrier(term_text.astype(jnp.bfloat16)).astype(jnp.float32)
        term_image = lax.optimization_barrier(term_image.astype(jnp.bfloat16)).astype(jnp.float32)
        return (totals[0] + term_text, totals[1] + term_image)

    start_grads = (jnp.zeros((D, FF), jnp.float32), jnp.zeros((D, FF), jnp.float32))
    grad_down_text, grad_down_image = lax.fori_loop(0, N_FSDP, grad_block, start_grads)
    return (ref_out, grad_gate, grad_up, grad_down_text, grad_down_image)
```

```python
import jax
import jax.numpy as jnp
from jax import lax
from jax.sharding import PartitionSpec as P

dpo_beta = 0.1
bf16 = jnp.bfloat16
f32 = jnp.float32
BOTH = ("fsdp", "tp")


def pairs_of(move):
    pairs = []
    for zl in range(2):
        for x in range(4):
            for y in range(4):
                for zh in range(2):
                    for c in range(2):
                        x2, zl2, y2, zh2, c2 = move(x, zl, y, zh, c)
                        src = (zl * 4 + x) * 16 + y * 4 + zh * 2 + c
                        dst = (zl2 * 4 + x2) * 16 + y2 * 4 + zh2 * 2 + c2
                        pairs.append((src, dst))
    return pairs


X_UP = pairs_of(lambda x, zl, y, zh, c: ((x + 1) % 4, zl, y, zh, c))
X_DOWN = pairs_of(lambda x, zl, y, zh, c: ((x + 3) % 4, zl, y, zh, c))
X_OPP = pairs_of(lambda x, zl, y, zh, c: ((x + 2) % 4, zl, y, zh, c))
Y_UP = pairs_of(lambda x, zl, y, zh, c: (x, zl, (y + 1) % 4, zh, c))
Y_DOWN = pairs_of(lambda x, zl, y, zh, c: (x, zl, (y + 3) % 4, zh, c))
ZL_FLIP = pairs_of(lambda x, zl, y, zh, c: (x, 1 - zl, y, zh, c))
ZH_FLIP = pairs_of(lambda x, zl, y, zh, c: (x, zl, y, 1 - zh, c))
C_FLIP = pairs_of(lambda x, zl, y, zh, c: (x, zl, y, zh, 1 - c))
SWAP = pairs_of(
    lambda x, zl, y, zh, c: ((y % 2) * 2 + zh, zl, (y // 2) * 2 + x // 2, x % 2, c)
)


def send(value, pairs):
    return lax.ppermute(value, BOTH, pairs)


def ring_gather(lo, hi, up, down):
    below_lo = send(lo, up)
    above_hi = send(hi, down)
    below_hi = send(hi, up)
    above_lo = send(lo, down)
    opp_lo = send(below_lo, up)
    opp_hi = send(above_hi, down)
    return (below_lo, below_hi), (above_lo, above_hi), (opp_lo, opp_hi)


def ring_scatter(opp, above, below, own, up, down):
    via_lo = send(opp[0], up)
    via_hi = send(opp[1], down)
    got_a_hi = send(above[1], up)
    got_b_lo = send(below[0], down)
    got_a_lo = send((above[0].astype(f32) + via_lo.astype(f32)).astype(bf16), up)
    got_b_hi = send((below[1].astype(f32) + via_hi.astype(f32)).astype(bf16), down)
    lo = own[0].astype(f32) + got_b_lo.astype(f32) + got_a_lo.astype(f32)
    hi = own[1].astype(f32) + got_a_hi.astype(f32) + got_b_hi.astype(f32)
    return lo, hi


def put(buf, value, *start):
    zero = jnp.int32(0)
    index = tuple(jnp.int32(s) for s in start) + (zero,) * (buf.ndim - len(start))
    return lax.dynamic_update_slice(buf, value, index)


def gather_hidden(hidden, x):
    half = hidden.shape[0] // 2
    lo, hi = hidden[:half], hidden[half:]
    below, above, opp = ring_gather(lo, hi, X_UP, X_DOWN)
    buf = jnp.zeros((4, 2, half, hidden.shape[1]), bf16)
    buf = put(buf, hidden.reshape(1, 2, half, -1), x)
    for at, part in (((x + 3) % 4, below), ((x + 1) % 4, above), ((x + 2) % 4, opp)):
        buf = put(buf, part[0][None, None], at, 0)
        buf = put(buf, part[1][None, None], at, 1)
    return buf.reshape(4 * hidden.shape[0], hidden.shape[1])


def per_device(
    ref_gate,
    ref_up,
    ref_residual,
    ref_modality,
    ref_down_text,
    ref_down_image,
    pol_gate,
    pol_up,
    pol_modality,
    pol_segment,
    pair_margin,
    token_cotangent,
    pol_down_text,
    pol_down_image,
):
    fi = lax.axis_index("fsdp")
    ti = lax.axis_index("tp")
    zl, x = fi // 4, fi % 4
    y, zh, c = ti // 4, (ti // 2) % 2, ti % 2
    rows = ref_gate.shape[0]
    cols = token_cotangent.shape[1]

    seg_ids = jnp.arange(2 * pair_margin.shape[0], dtype=jnp.int32)
    pair_weight = dpo_beta * jax.nn.sigmoid(-dpo_beta * pair_margin)
    table = jnp.repeat(pair_weight, 2) * jnp.where(seg_ids % 2 == 0, -1.0, 1.0).astype(f32)
    coef = jnp.sum(
        jnp.where(pol_segment[:, None] == seg_ids[None, :], table[None, :], f32(0.0)), axis=1
    )
    local_cot = (coef[:, None] * token_cotangent.astype(f32)).astype(bf16)
    moved_cot = send(local_cot, SWAP)

    r_rt, r_ri = send(ref_down_text, ZL_FLIP), send(ref_down_image, ZL_FLIP)
    r_pt, r_pi = send(pol_down_text, ZL_FLIP), send(pol_down_image, ZL_FLIP)

    mods = jnp.stack([ref_modality, pol_modality])
    m_below, m_above, m_opp = send(mods, X_UP), send(mods, X_DOWN), send(mods, X_OPP)
    mod_buf = jnp.zeros((4, 2, rows), jnp.int32)
    for at, part in (((x + 3) % 4, m_below), ((x + 1) % 4, m_above), ((x + 2) % 4, m_opp), (x, mods)):
        mod_buf = put(mod_buf, part[None], at)
    ref_img = (mod_buf[:, 0].reshape(-1) == 1)[:, None]
    pol_img = (mod_buf[:, 1].reshape(-1) == 1)[:, None]

    gate_r = ref_gate.astype(f32)
    h_ref = (gate_r * jax.nn.sigmoid(gate_r) * ref_up.astype(f32)).astype(bf16)
    gate_p, up_p = pol_gate.astype(f32), pol_up.astype(f32)
    sig = jax.nn.sigmoid(gate_p)
    act = gate_p * sig
    h_pol = (act * up_p).astype(bf16)
    all_ref = gather_hidden(h_ref, x)
    all_pol = gather_hidden(h_pol, x)

    other_zh = send(moved_cot, ZH_FLIP)
    c_lo = jnp.where(zh == 0, moved_cot, other_zh)
    c_hi = jnp.where(zh == 0, other_zh, moved_cot)
    below, above, opp = ring_gather(c_lo, c_hi, Y_UP, Y_DOWN)
    cot_buf = jnp.zeros((2, 4, rows, 2 * cols), bf16)
    for at, part in ((y, (c_lo, c_hi)), ((y + 3) % 4, below), ((y + 1) % 4, above), ((y + 2) % 4, opp)):
        for k in range(2):
            mine = part[k]
            theirs = send(mine, C_FLIP)
            both = jnp.concatenate(
                [jnp.where(c == 0, mine, theirs), jnp.where(c == 0, theirs, mine)], axis=1
            )
            cot_buf = put(cot_buf, both[None, None], (at // 2) ^ zl, (at % 2) * 2 + k)
    cot_own = cot_buf[0].reshape(4 * rows, 2 * cols)
    cot_far = cot_buf[1].reshape(4 * rows, 2 * cols)

    contract = (((1,), (1,)), ((), ()))
    zero = jnp.zeros_like(all_ref)
    ref_t, ref_i = jnp.where(ref_img, zero, all_ref), jnp.where(ref_img, all_ref, zero)

    def forward(wt, wi):
        return lax.dot_general(ref_t, wt, contract, preferred_element_type=f32) + lax.dot_general(
            ref_i, wi, contract, preferred_element_type=f32
        )

    quarter = []
    for wt, wi in ((ref_down_text, ref_down_image), (r_rt, r_ri)):
        away = (1 - c) * cols
        kept = c * cols
        out_away = forward(
            lax.dynamic_slice_in_dim(wt, away, cols, 0), lax.dynamic_slice_in_dim(wi, away, cols, 0)
        ).astype(bf16)
        got = send(out_away, C_FLIP)
        out_kept = forward(
            lax.dynamic_slice_in_dim(wt, kept, cols, 0), lax.dynamic_slice_in_dim(wi, kept, cols, 0)
        )
        quarter.append((out_kept + got.astype(f32)).astype(bf16))
    partial = jnp.stack(quarter).reshape(2, 4, rows, cols)

    def share(at):
        r, yl = (at // 2) ^ zl, at % 2
        zero_i = jnp.int32(0)
        both = lax.dynamic_slice(partial, (r, yl * 2, zero_i, zero_i), (1, 2, rows, cols))
        return both[0, 0], both[0, 1]

    lo, hi = ring_scatter(
        share((y + 2) % 4), share((y + 1) % 4), share((y + 3) % 4), share(y), Y_UP, Y_DOWN
    )
    zh_away = jnp.where(zh == 0, hi, lo).astype(bf16)
    zh_kept = jnp.where(zh == 0, lo, hi)
    summed = (zh_kept + send(zh_away, ZH_FLIP).astype(f32)).astype(bf16)
    ref_out = (send(summed, SWAP).astype(f32) + ref_residual.astype(f32)).astype(bf16)

    zc = jnp.zeros_like(cot_own)
    own_t, own_i = jnp.where(pol_img, zc, cot_own), jnp.where(pol_img, cot_own, zc)
    far_t, far_i = jnp.where(pol_img, zc, cot_far), jnp.where(pol_img, cot_far, zc)
    d_part = jnp.dot(own_t, pol_down_text, preferred_element_type=f32)
    d_part = d_part + jnp.dot(own_i, pol_down_image, preferred_element_type=f32)
    d_part = d_part + jnp.dot(far_t, r_pt, preferred_element_type=f32)
    d_part = d_part + jnp.dot(far_i, r_pi, preferred_element_type=f32)
    d_part = d_part.astype(bf16).reshape(4, 2, rows // 2, -1)

    def d_share(at):
        both = lax.dynamic_index_in_dim(d_part, at, 0, keepdims=False)
        return both[0], both[1]

    d_lo, d_hi = ring_scatter(
        d_share((x + 2) % 4), d_share((x + 1) % 4), d_share((x + 3) % 4), d_share(x), X_UP, X_DOWN
    )
    d_hidden = jnp.concatenate([d_lo, d_hi], axis=0)
    grad_gate = (d_hidden * up_p * sig * (1.0 + gate_p * (1.0 - sig))).astype(bf16)
    grad_up = (d_hidden * act).astype(bf16)

    over_rows = (((0,), (0,)), ((), ()))
    zp = jnp.zeros_like(all_pol)
    pol_t, pol_i = jnp.where(pol_img, zp, all_pol), jnp.where(pol_img, all_pol, zp)
    grads = []
    for h in (pol_t, pol_i):
        away = lax.dot_general(cot_far, h, over_rows, preferred_element_type=f32).astype(bf16)
        got = send(away, ZL_FLIP)
        kept = lax.dot_general(cot_own, h, over_rows, preferred_element_type=f32)
        grads.append(kept + got.astype(f32))
    return (ref_out, grad_gate, grad_up, grads[0], grads[1])


def solution(mesh):
    spec = P("fsdp", "tp")
    in_specs = (
        spec,
        spec,
        spec,
        P("fsdp"),
        spec,
        spec,
        spec,
        spec,
        P("fsdp"),
        P("fsdp"),
        P(),
        spec,
        spec,
        spec,
    )
    return jax.shard_map(
        per_device, mesh=mesh, in_specs=in_specs, out_specs=(spec,) * 5, check_vma=False
    )
```

```python
import jax
import jax.numpy as jnp
from jax import lax
from jax.sharding import PartitionSpec as P

dpo_beta = 0.1
bf16 = jnp.bfloat16
f32 = jnp.float32
BOTH = ("fsdp", "tp")


def pairs_of(move):
    pairs = []
    for zl in range(2):
        for x in range(4):
            for y in range(4):
                for zh in range(2):
                    for c in range(2):
                        x2, zl2, y2, zh2, c2 = move(x, zl, y, zh, c)
                        src = (zl * 4 + x) * 16 + y * 4 + zh * 2 + c
                        dst = (zl2 * 4 + x2) * 16 + y2 * 4 + zh2 * 2 + c2
                        pairs.append((src, dst))
    return pairs


X_UP = pairs_of(lambda x, zl, y, zh, c: ((x + 1) % 4, zl, y, zh, c))
X_DOWN = pairs_of(lambda x, zl, y, zh, c: ((x + 3) % 4, zl, y, zh, c))
X_OPP = pairs_of(lambda x, zl, y, zh, c: ((x + 2) % 4, zl, y, zh, c))
Y_UP = pairs_of(lambda x, zl, y, zh, c: (x, zl, (y + 1) % 4, zh, c))
Y_DOWN = pairs_of(lambda x, zl, y, zh, c: (x, zl, (y + 3) % 4, zh, c))
ZL_FLIP = pairs_of(lambda x, zl, y, zh, c: (x, 1 - zl, y, zh, c))
ZH_FLIP = pairs_of(lambda x, zl, y, zh, c: (x, zl, y, 1 - zh, c))
C_FLIP = pairs_of(lambda x, zl, y, zh, c: (x, zl, y, zh, 1 - c))


def to_rows_owner(x, zl, y, zh, c):
    x2 = (y % 2) * 2 + zh
    d = (x - x2) % 4
    return x2, zl, ((y // 2) ^ zl) * 2 + d // 2, d % 2, c


TO_ROWS = pairs_of(to_rows_owner)
FROM_ROWS = [(dst, src) for src, dst in TO_ROWS]


def send(value, pairs):
    return lax.ppermute(value, BOTH, pairs)


def ring_gather(own, axis, up, down):
    half = own.shape[axis] // 2
    below = send(own, up)
    above = send(own, down)
    opp_lo = send(lax.slice_in_dim(below, 0, half, axis=axis), up)
    opp_hi = send(lax.slice_in_dim(above, half, 2 * half, axis=axis), down)
    return above, jnp.concatenate([opp_lo, opp_hi], axis=axis), below


def ring_scatter(opp, above, below, own, up, down):
    half = opp.shape[0] // 2
    via_lo = send(opp[:half], up)
    via_hi = send(opp[half:], down)
    above = jnp.concatenate(
        [(above[:half].astype(f32) + via_lo.astype(f32)).astype(bf16), above[half:]], axis=0
    )
    below = jnp.concatenate(
        [below[:half], (below[half:].astype(f32) + via_hi.astype(f32)).astype(bf16)], axis=0
    )
    got_a, got_b = send(above, up), send(below, down)
    return own.astype(f32) + got_a.astype(f32) + got_b.astype(f32)


def per_device(
    ref_gate,
    ref_up,
    ref_residual,
    ref_modality,
    ref_down_text,
    ref_down_image,
    pol_gate,
    pol_up,
    pol_modality,
    pol_segment,
    pair_margin,
    token_cotangent,
    pol_down_text,
    pol_down_image,
):
    fi = lax.axis_index("fsdp")
    ti = lax.axis_index("tp")
    zl = fi // 4
    y, zh, c = ti // 4, (ti // 2) % 2, ti % 2
    rows = ref_gate.shape[0]
    cols = token_cotangent.shape[1]
    zero_i = jnp.int32(0)

    seg_ids = jnp.arange(2 * pair_margin.shape[0], dtype=jnp.int32)
    pair_weight = dpo_beta * jax.nn.sigmoid(-dpo_beta * pair_margin)
    table = jnp.repeat(pair_weight, 2) * jnp.where(seg_ids % 2 == 0, -1.0, 1.0).astype(f32)
    coef = jnp.sum(
        jnp.where(pol_segment[:, None] == seg_ids[None, :], table[None, :], f32(0.0)), axis=1
    )
    local_cot = (coef[:, None] * token_cotangent.astype(f32)).astype(bf16)
    moved_cot = send(local_cot, TO_ROWS)

    rt, ri = ref_down_text.T, ref_down_image.T
    far_rt, far_ri = send(rt, ZL_FLIP), send(ri, ZL_FLIP)
    pol_w = jnp.concatenate([pol_down_text.T, pol_down_image.T], axis=1)
    far_pol_w = send(pol_w, ZL_FLIP)

    mods = jnp.stack([ref_modality, pol_modality])
    mods = jnp.stack([mods, send(mods, X_DOWN), send(mods, X_OPP), send(mods, X_UP)])
    ref_img = mods[:, 0][:, None, :] == 1
    pol_img = mods[:, 1].reshape(2, 2 * rows, 1) == 1

    gate_r = ref_gate.T.astype(f32)
    h_ref = (gate_r * jax.nn.sigmoid(gate_r) * ref_up.T.astype(f32)).astype(bf16)
    gate_p, up_p = pol_gate.T.astype(f32), pol_up.T.astype(f32)
    sig = jax.nn.sigmoid(gate_p)
    act = gate_p * sig
    h_pol = (act * up_p).astype(bf16)
    all_ref = (h_ref, *ring_gather(h_ref, 1, X_UP, X_DOWN))
    all_pol = (h_pol, *ring_gather(h_pol, 1, X_UP, X_DOWN))

    other_zh = send(moved_cot, ZH_FLIP)
    own_cot = jnp.concatenate(
        [jnp.where(zh == 0, moved_cot, other_zh), jnp.where(zh == 0, other_zh, moved_cot)], axis=0
    )
    pieces = (own_cot, *ring_gather(own_cot, 0, Y_UP, Y_DOWN))
    cot_buf = jnp.zeros((2, 2, 2 * rows, 4 * cols), bf16)
    for step in (0, 1, 3, 2):
        mine = pieces[step]
        theirs = send(mine, C_FLIP)
        at = (y + step) % 4
        r, yl = at // 2, at % 2
        both = jnp.concatenate(
            [jnp.where(c == 0, mine, theirs), jnp.where(c == 0, theirs, mine)], axis=1
        )
        img = jnp.where(yl == 0, pol_img[0], pol_img[1])
        none = jnp.zeros_like(both)
        both = jnp.concatenate([jnp.where(img, none, both), jnp.where(img, both, none)], axis=1)
        cot_buf = lax.dynamic_update_slice(cot_buf, both[None, None], (r, yl, zero_i, zero_i))
    cot = cot_buf.reshape(2, 4, rows, 4 * cols)

    over_first = (((0,), (0,)), ((), ()))

    def forward(h, img, wt, wi):
        none = jnp.zeros_like(h)
        return lax.dot_general(
            jnp.where(img, none, h), wt, over_first, preferred_element_type=f32
        ) + lax.dot_general(jnp.where(img, h, none), wi, over_first, preferred_element_type=f32)

    def halves(w):
        first, second = w[:, :cols], w[:, cols:]
        return jnp.where(c == 0, first, second), jnp.where(c == 0, second, first)

    kept_t, away_t = zip(halves(rt), halves(far_rt))
    kept_i, away_i = zip(halves(ri), halves(far_ri))
    away_t, away_i = jnp.concatenate(away_t, axis=1), jnp.concatenate(away_i, axis=1)
    kept_t, kept_i = jnp.concatenate(kept_t, axis=1), jnp.concatenate(kept_i, axis=1)
    by_piece = []
    for d in (0, 1, 3, 2):
        got = send(forward(all_ref[d], ref_img[d], away_t, away_i).astype(bf16), C_FLIP)
        kept = forward(all_ref[d], ref_img[d], kept_t, kept_i) + got.astype(f32)
        by_piece.append(kept.astype(bf16))
    by_piece = (by_piece[0], by_piece[1], by_piece[3], by_piece[2])
    shares = jnp.stack(
        [
            jnp.concatenate([by_piece[2 * yl + k][:, r * cols : (r + 1) * cols] for k in range(2)], axis=0)
            for r in range(2)
            for yl in range(2)
        ]
    )

    def share(step):
        return lax.dynamic_index_in_dim(shares, (y + step) % 4, 0, keepdims=False)

    total = ring_scatter(share(2), share(1), share(3), share(0), Y_UP, Y_DOWN)
    lo, hi = total[:rows], total[rows:]
    zh_away = jnp.where(zh == 0, hi, lo).astype(bf16)
    zh_kept = jnp.where(zh == 0, lo, hi)
    summed = (zh_kept + send(zh_away, ZH_FLIP).astype(f32)).astype(bf16)
    ref_out = (send(summed, FROM_ROWS).astype(f32) + ref_residual.astype(f32)).astype(bf16)

    over_last = (((1,), (1,)), ((), ()))

    def backward(d):
        near = lax.dot_general(pol_w, cot[0, d], over_last, preferred_element_type=f32)
        far = lax.dot_general(far_pol_w, cot[1, d], over_last, preferred_element_type=f32)
        return (near + far).astype(bf16)

    d_hidden = ring_scatter(backward(2), backward(1), backward(3), backward(0), X_UP, X_DOWN)
    grad_gate = (d_hidden * up_p * sig * (1.0 + gate_p * (1.0 - sig))).astype(bf16)
    grad_up = (d_hidden * act).astype(bf16)

    def down(r):
        return sum(
            jnp.dot(all_pol[d], cot[r, d], preferred_element_type=f32) for d in (0, 1, 3, 2)
        )

    got = send(down(1).astype(bf16), ZL_FLIP)
    grads = down(0) + got.astype(f32)
    width = 2 * cols
    return (ref_out, grad_gate.T, grad_up.T, grads[:, :width].T, grads[:, width:].T)


def solution(mesh):
    spec = P("fsdp", "tp")
    in_specs = (
        spec,
        spec,
        spec,
        P("fsdp"),
        spec,
        spec,
        spec,
        spec,
        P("fsdp"),
        P("fsdp"),
        P(),
        spec,
        spec,
        spec,
    )
    return jax.shard_map(
        per_device, mesh=mesh, in_specs=in_specs, out_specs=(spec,) * 5, check_vma=False
    )
```

```python
import jax
import jax.numpy as jnp
from jax import lax
from jax.experimental import pallas as pl
from jax.experimental.pallas import tpu as pltpu
from jax.sharding import PartitionSpec as P

dpo_beta = 0.1
bf16 = jnp.bfloat16
f32 = jnp.float32
MESH = pl.DeviceIdType.MESH


N_SEM = 48


def lanes(n, width=256):
    return pl.ds(pl.multiple_of(n * width, width), width)


def loop(count, body):
    def step(n, carry):
        body(n)
        return carry

    lax.fori_loop(0, count, step, 0)


def step_kernel(
    cot_in,
    mod_in,
    href_in,
    wref_in,
    hpol_in,
    wpol_in,
    out_ref,
    out_d,
    out_w,
    hr,
    hp,
    wr,
    wp,
    cr,
    mods,
    hs,
    cs,
    aw,
    ar,
    kp,
    sr,
    va,
    vb,
    ga,
    gb,
    za,
    zr,
    fo,
    dh,
    xa_via,
    xb_via,
    xa,
    xb,
    dws,
    dwr,
    send_sems,
    recv_sems,
    local_sems,
):
    fi = lax.axis_index("fsdp")
    ti = lax.axis_index("tp")
    zl, x = fi // 4, fi % 4
    y, zh, c = ti // 4, (ti // 2) % 2, ti % 2
    ff, rows = href_in.shape
    cols = cot_in.shape[0]
    cut = (ff // 32) * 16
    tiles = rows // 256

    def device(x2, zl2, y2, zh2, c2):
        return (zl2 * 4 + x2, y2 * 4 + zh2 * 2 + c2)

    x_up, x_down = device((x + 1) % 4, zl, y, zh, c), device((x + 3) % 4, zl, y, zh, c)
    x_opp = device((x + 2) % 4, zl, y, zh, c)
    y_up, y_down = device(x, zl, (y + 1) % 4, zh, c), device(x, zl, (y + 3) % 4, zh, c)
    zl_flip, zh_flip = device(x, 1 - zl, y, zh, c), device(x, zl, y, 1 - zh, c)
    c_flip = device(x, zl, y, zh, 1 - c)
    rows_x = (y % 2) * 2 + zh
    rows_d = (x - rows_x + 4) % 4
    rows_y = ((y // 2 + zl) % 2) * 2 + rows_d // 2
    rows_dev = device(rows_x, zl, rows_y, rows_d % 2, c)
    rows_k = rows_y * 2 + rows_d % 2
    back_d = (y % 2) * 2 + zh
    back_dev = device((x + back_d) % 4, zl, ((y // 2 + zl) % 2) * 2 + x // 2, x % 2, c)
    stays = jnp.logical_and(rows_dev[0] == fi, rows_dev[1] == ti)
    moves = jnp.logical_not(stays)

    barrier = pltpu.get_barrier_semaphore()
    for dev in (x_up, x_down, x_opp, y_up, y_down, zl_flip, zh_flip, c_flip):
        pl.semaphore_signal(barrier, inc=1, device_id=dev, device_id_type=MESH)

    @pl.when(moves)
    def _():
        for dev in (rows_dev, back_dev):
            pl.semaphore_signal(barrier, inc=1, device_id=dev, device_id_type=MESH)

    pl.semaphore_wait(barrier, jnp.where(moves, 10, 8))

    started = []

    def copy(src, dst, dev):
        n = len(started)
        rdma = pltpu.make_async_remote_copy(
            src_ref=src,
            dst_ref=dst,
            send_sem=send_sems.at[n],
            recv_sem=recv_sems.at[n],
            device_id=dev,
            device_id_type=MESH,
        )
        started.append(rdma)
        rdma.start()
        return rdma

    def copy_or_stay(n, src, dst, dst_here, dev):
        rdma = pltpu.make_async_remote_copy(
            src_ref=src,
            dst_ref=dst,
            send_sem=send_sems.at[n],
            recv_sem=recv_sems.at[n],
            device_id=dev,
            device_id_type=MESH,
        )
        here = pltpu.make_async_copy(src, dst_here, local_sems.at[n - N_SEM])

        @pl.when(moves)
        def _():
            rdma.start()

        @pl.when(stays)
        def _():
            here.start()

        def wait():
            @pl.when(moves)
            def _():
                rdma.wait()

            @pl.when(stays)
            def _():
                here.wait()

        return wait

    def local(n, src, dst):
        here = pltpu.make_async_copy(src, dst, local_sems.at[n])
        here.start()
        return here

    k_own = y * 2 + zh
    wait_moved = copy_or_stay(N_SEM, cot_in, cr.at[c, rows_k], cr.at[c, k_own], rows_dev)
    m_up = copy(mod_in, mods.at[3], x_up)
    m_down = copy(mod_in, mods.at[1], x_down)
    m_opp = copy(mod_in, mods.at[2], x_opp)
    h_up = copy(href_in, hr.at[3], x_up)
    h_down = copy(href_in, hr.at[1], x_down)
    half = wref_in.shape[0] // 2
    w_lo = copy(wref_in.at[pl.ds(0, half)], wr.at[1, pl.ds(0, half)], zl_flip)
    own = [
        local(2, mod_in, mods.at[0]),
        local(3, href_in, hr.at[0]),
        local(4, wref_in, wr.at[0]),
        local(5, hpol_in, hp.at[0]),
        local(6, wpol_in, wp.at[0]),
    ]

    wait_moved()
    cot_zh = copy(cr.at[c, k_own], cr.at[c, k_own], zh_flip)
    w_hi = copy(wref_in.at[pl.ds(half, half)], wr.at[1, pl.ds(half, half)], zl_flip)
    for here in own:
        here.wait()
    cot_zh.wait_recv()
    pair = cr.at[c, pl.ds(y * 2, 2)]
    cot_up = copy(pair, pair, y_up)
    cot_down = copy(pair, pair, y_down)
    wp_far = copy(wpol_in, wp.at[1], zl_flip)
    cot_c = [copy(pair, pair, c_flip)]

    h_up.wait_recv()
    h_down.wait_recv()
    lo, hi = pl.ds(0, cut), pl.ds(cut, ff - cut)
    h_opp_lo = copy(hr.at[3, lo], hr.at[2, lo], x_up)
    h_opp_hi = copy(hr.at[1, hi], hr.at[2, hi], x_down)
    p_up = copy(hpol_in, hp.at[3], x_up)
    p_down = copy(hpol_in, hp.at[1], x_down)
    m_up.wait_recv()
    m_down.wait_recv()
    m_opp.wait_recv()

    below, above, opp = (y + 3) % 4, (y + 1) % 4, (y + 2) % 4

    def image(d, row, where):
        return mods[d, pl.ds(row, 1), where].astype(bf16)

    def ref_piece(d, slot):
        def tile(n):
            where = lanes(n)
            img = image(d, 0, where)
            block = hr[d, :, where]
            hs[pl.ds(0, ff)] = block * (1 - img)
            hs[pl.ds(ff, ff)] = block * img
            for r in range(2):
                there = pl.ds(pl.multiple_of((1 - c) * cols, cols), cols)
                away = jnp.dot(wr[r, there], hs[...], preferred_element_type=f32)
                aw[d, r, :, where] = away.astype(bf16)
                stay = pl.ds(pl.multiple_of(c * cols, cols), cols)
                kp[slot, r, :, where] = jnp.dot(wr[r, stay], hs[...], preferred_element_type=f32)

        loop(tiles, tile)
        return copy(aw.at[d], ar.at[d], c_flip)

    def ref_sum(d, slot, got):
        got.wait_recv()

        def tile(n):
            where = lanes(n)
            for r in range(2):
                total = kp[slot, r, :, where] + ar[d, r, :, where].astype(f32)
                sr[r * 4 + d, :, where] = total.astype(bf16)

        loop(tiles, tile)

    w_lo.wait_recv()
    w_hi.wait_recv()
    got0 = ref_piece(0, 0)

    cot_up.wait_recv()
    cot_down.wait_recv()
    cot_opp_lo = copy(cr.at[c, below * 2], cr.at[c, below * 2], y_up)
    cot_opp_hi = copy(cr.at[c, above * 2 + 1], cr.at[c, above * 2 + 1], y_down)
    for at in (below, above):
        other = cr.at[c, pl.ds(at * 2, 2)]
        cot_c.append(copy(other, other, c_flip))

    got1 = ref_piece(1, 1)
    ref_sum(0, 0, got0)
    got3 = ref_piece(3, 0)
    ref_sum(1, 1, got1)
    h_opp_lo.wait_recv()
    h_opp_hi.wait_recv()
    got2 = ref_piece(2, 1)
    ref_sum(3, 0, got3)
    ref_sum(2, 1, got2)

    via_up = copy(sr.at[opp * 2], va, y_up)
    via_down = copy(sr.at[opp * 2 + 1], vb, y_down)
    first_up = copy(sr.at[above * 2 + 1], ga.at[1], y_up)
    first_down = copy(sr.at[below * 2], gb.at[0], y_down)

    cot_opp_lo.wait_recv()
    cot_opp_hi.wait_recv()
    other = cr.at[c, pl.ds(opp * 2, 2)]
    cot_c.append(copy(other, other, c_flip))

    p_up.wait_recv()
    p_down.wait_recv()
    p_opp_lo = copy(hp.at[3, lo], hp.at[2, lo], x_up)
    p_opp_hi = copy(hp.at[1, hi], hp.at[2, hi], x_down)

    via_up.wait_recv()
    via_down.wait_recv()

    def add_via(n):
        where = lanes(n)
        for at, via in ((above * 2, va), (below * 2 + 1, vb)):
            total = sr[at, :, where].astype(f32) + via[:, where].astype(f32)
            sr[at, :, where] = total.astype(bf16)

    loop(tiles, add_via)
    last_up = copy(sr.at[above * 2], ga.at[0], y_up)
    last_down = copy(sr.at[below * 2 + 1], gb.at[1], y_down)

    for got in cot_c:
        got.wait_recv()
    wp_far.wait_recv()

    def d_piece(d, store):
        def tile(n):
            where = lanes(n)
            img = image(d, 1, where)
            for r in range(2):
                for core in range(2):
                    block = cr[core, r * 4 + d, :, where]
                    at = r * 4 * cols + core * cols
                    cs[pl.ds(at, cols)] = block * (1 - img)
                    cs[pl.ds(at + 2 * cols, cols)] = block * img
            part = jnp.dot(wp[0], cs[pl.ds(0, 4 * cols)], preferred_element_type=f32)
            part += jnp.dot(wp[1], cs[pl.ds(4 * cols, 4 * cols)], preferred_element_type=f32)
            store(where, part)

        loop(tiles, tile)

    def store_dh(slot):
        def store(where, part):
            dh[slot, :, where] = part.astype(bf16)

        return store

    d_piece(2, store_dh(2))
    d_via_up = copy(dh.at[2, lo], xa_via, x_up)
    d_via_down = copy(dh.at[2, hi], xb_via, x_down)

    first_up.wait_recv()
    first_down.wait_recv()
    last_up.wait_recv()
    last_down.wait_recv()

    def y_sum(k, where):
        total = sr[y * 2 + k, :, where].astype(f32) + ga[k, :, where].astype(f32)
        return total + gb[k, :, where].astype(f32)

    def z_away(n):
        where = lanes(n)
        za[:, where] = y_sum(1 - zh, where).astype(bf16)

    loop(tiles, z_away)
    z_copy = copy(za, zr, zh_flip)

    p_opp_lo.wait_recv()
    p_opp_hi.wait_recv()

    def down(r, core, modality):
        total = None
        for d in range(4):
            img = image(d, 1, slice(None))
            block = cr[core, r * 4 + d] * (img if modality else 1 - img)
            part = lax.dot_general(
                hp[d], block, (((1,), (1,)), ((), ())), preferred_element_type=f32
            )
            total = part if total is None else total + part
        return total

    d_piece(1, store_dh(0))
    d_first_up = copy(dh.at[0, hi], xa.at[hi], x_up)
    d_piece(3, store_dh(1))
    d_first_down = copy(dh.at[1, lo], xb.at[lo], x_down)

    dw_sent = []
    for modality in range(2):

        def away(core, modality=modality):
            dws[modality, :, lanes(core)] = down(1, core, modality).astype(bf16)

        loop(2, away)
        dw_sent.append(copy(dws.at[modality], dwr.at[modality], zl_flip))

    d_via_up.wait_recv()
    d_via_down.wait_recv()

    def add_d(n):
        where = lanes(n)
        dh[0, lo, where] = (dh[0, lo, where].astype(f32) + xa_via[:, where].astype(f32)).astype(bf16)
        dh[1, hi, where] = (dh[1, hi, where].astype(f32) + xb_via[:, where].astype(f32)).astype(bf16)

    loop(tiles, add_d)
    d_last_up = copy(dh.at[0, lo], xa.at[lo], x_up)
    d_last_down = copy(dh.at[1, hi], xb.at[hi], x_down)

    z_copy.wait_recv()

    def z_sum(n):
        where = lanes(n)
        fo[:, where] = (y_sum(zh, where) + zr[:, where].astype(f32)).astype(bf16)

    loop(tiles, z_sum)
    wait_back = copy_or_stay(N_SEM + 1, fo, out_ref, out_ref, back_dev)

    def store_own(where, part):
        out_d[:, where] = part

    d_piece(0, store_own)

    for modality in range(2):
        for core in range(2):
            out_w[modality, :, pl.ds(core * cols, cols)] = down(0, core, modality)

    for got in (d_first_up, d_first_down, d_last_up, d_last_down):
        got.wait_recv()

    def d_sum(n):
        where = lanes(n)
        both = xa[:, where].astype(f32) + xb[:, where].astype(f32)
        out_d[:, where] = out_d[:, where] + both

    loop(tiles, d_sum)
    for modality in range(2):
        dw_sent[modality].wait_recv()

        def dw_sum(core, modality=modality):
            where = lanes(core)
            out_w[modality, :, where] = out_w[modality, :, where] + dwr[modality, :, where].astype(f32)

        loop(2, dw_sum)
    wait_back()
    for rdma in started:
        rdma.wait_send()


def communicate(cot, mod, href, wref, hpol, wpol):
    ff, rows = href.shape
    cols = cot.shape[0]
    depth = wref.shape[0]
    cut = (ff // 32) * 16
    vmem = pltpu.VMEM
    scratch = [
        vmem((4, ff, rows), bf16),
        vmem((4, ff, rows), bf16),
        vmem((2, depth, 2 * ff), bf16),
        vmem((2, ff, 2 * depth), bf16),
        vmem((2, 8, cols, rows), bf16),
        vmem((4, 8, rows), f32),
        vmem((2 * ff, 256), bf16),
        vmem((8 * cols, 256), bf16),
        vmem((4, 2, cols, rows), bf16),
        vmem((4, 2, cols, rows), bf16),
        vmem((2, 2, cols, rows), f32),
        vmem((8, cols, rows), bf16),
        vmem((cols, rows), bf16),
        vmem((cols, rows), bf16),
        vmem((2, cols, rows), bf16),
        vmem((2, cols, rows), bf16),
        vmem((cols, rows), bf16),
        vmem((cols, rows), bf16),
        vmem((cols, rows), bf16),
        vmem((3, ff, rows), bf16),
        vmem((cut, rows), bf16),
        vmem((ff - cut, rows), bf16),
        vmem((ff, rows), bf16),
        vmem((ff, rows), bf16),
        vmem((2, ff, depth), bf16),
        vmem((2, ff, depth), bf16),
        pltpu.SemaphoreType.DMA((N_SEM + 2,)),
        pltpu.SemaphoreType.DMA((N_SEM + 2,)),
        pltpu.SemaphoreType.DMA((8,)),
    ]
    anywhere = pl.BlockSpec(memory_space=pl.ANY)
    in_vmem = pl.BlockSpec(memory_space=vmem)
    return pl.pallas_call(
        step_kernel,
        out_shape=(
            jax.ShapeDtypeStruct((cols, rows), bf16),
            jax.ShapeDtypeStruct((ff, rows), f32),
            jax.ShapeDtypeStruct((2, ff, depth), f32),
        ),
        in_specs=[anywhere] * 6,
        out_specs=(in_vmem,) * 3,
        scratch_shapes=scratch,
        compiler_params=pltpu.CompilerParams(
            collective_id=0, has_side_effects=True, vmem_limit_bytes=66_000_000
        ),
    )(cot, mod, href, wref, hpol, wpol)


def per_device(
    ref_gate,
    ref_up,
    ref_residual,
    ref_modality,
    ref_down_text,
    ref_down_image,
    pol_gate,
    pol_up,
    pol_modality,
    pol_segment,
    pair_margin,
    token_cotangent,
    pol_down_text,
    pol_down_image,
):
    rows = ref_gate.shape[0]
    seg_ids = jnp.arange(2 * pair_margin.shape[0], dtype=jnp.int32)
    pair_weight = dpo_beta * jax.nn.sigmoid(-dpo_beta * pair_margin)
    table = jnp.repeat(pair_weight, 2) * jnp.where(seg_ids % 2 == 0, -1.0, 1.0).astype(f32)
    coef = jnp.sum(
        jnp.where(pol_segment[None, :] == seg_ids[:, None], table[:, None], f32(0.0)), axis=0
    )
    cot = (coef[None, :] * token_cotangent.T.astype(f32)).astype(bf16)
    mod = jnp.stack([ref_modality == 1, pol_modality == 1]).astype(f32)
    mod = jnp.concatenate([mod, jnp.zeros((6, rows), f32)], axis=0)

    gate_r = ref_gate.T.astype(f32)
    h_ref = (gate_r * jax.nn.sigmoid(gate_r) * ref_up.T.astype(f32)).astype(bf16)
    gate_p, up_p = pol_gate.T.astype(f32), pol_up.T.astype(f32)
    sig = jax.nn.sigmoid(gate_p)
    act = gate_p * sig
    h_pol = (act * up_p).astype(bf16)
    w_ref = jnp.concatenate([ref_down_text, ref_down_image], axis=1)
    w_pol = jnp.concatenate([pol_down_text.T, pol_down_image.T], axis=1)

    summed, d_hidden, grads = communicate(cot, mod, h_ref, w_ref, h_pol, w_pol)
    ref_out = (summed.T.astype(f32) + ref_residual.astype(f32)).astype(bf16)
    grad_gate = (d_hidden * up_p * sig * (1.0 + gate_p * (1.0 - sig))).astype(bf16)
    grad_up = (d_hidden * act).astype(bf16)
    return (ref_out, grad_gate.T, grad_up.T, grads[0].T, grads[1].T)


def solution(mesh):
    spec = P("fsdp", "tp")
    in_specs = (
        spec,
        spec,
        spec,
        P("fsdp"),
        spec,
        spec,
        spec,
        spec,
        P("fsdp"),
        P("fsdp"),
        P(),
        spec,
        spec,
        spec,
    )
    return jax.shard_map(
        per_device, mesh=mesh, in_specs=in_specs, out_specs=(spec,) * 5, check_vma=False
    )
```

```python
import jax
import jax.numpy as jnp
from jax import lax
from jax.experimental import pallas as pl
from jax.experimental.pallas import tpu as pltpu
from jax.sharding import PartitionSpec as P

dpo_beta = 0.1
bf16 = jnp.bfloat16
f32 = jnp.float32
MESH = pl.DeviceIdType.MESH


N_SEM = 64


def lanes(n, width=256):
    return pl.ds(pl.multiple_of(n * width, width), width)


def loop(count, body):
    def step(n, carry):
        body(n)
        return carry

    lax.fori_loop(0, count, step, 0)


def step_kernel(
    cot_in,
    mod_in,
    gate_r_in,
    up_r_in,
    gate_p_in,
    up_p_in,
    wref_in,
    wpol_t_in,
    wpol_i_in,
    out_ref,
    out_gate,
    out_up,
    out_t,
    out_i,
    gates,
    turned,
    d_own,
    hr,
    hp,
    wr,
    wp,
    cr,
    mods,
    hs,
    cs,
    aw,
    ar,
    kp,
    sr,
    va,
    vb,
    ga,
    gb,
    za,
    zr,
    fo,
    dh,
    xa_via,
    xb_via,
    xa,
    xb,
    dws,
    dwr,
    send_sems,
    recv_sems,
    local_sems,
):
    fi = lax.axis_index("fsdp")
    ti = lax.axis_index("tp")
    zl, x = fi // 4, fi % 4
    y, zh, c = ti // 4, (ti // 2) % 2, ti % 2
    ff, rows = gate_r_in.shape
    cols = cot_in.shape[0]
    cut = (ff // 32) * 16
    tiles = rows // 256

    def device(x2, zl2, y2, zh2, c2):
        return (zl2 * 4 + x2, y2 * 4 + zh2 * 2 + c2)

    x_up, x_down = device((x + 1) % 4, zl, y, zh, c), device((x + 3) % 4, zl, y, zh, c)
    x_opp = device((x + 2) % 4, zl, y, zh, c)
    y_up, y_down = device(x, zl, (y + 1) % 4, zh, c), device(x, zl, (y + 3) % 4, zh, c)
    zl_flip, zh_flip = device(x, 1 - zl, y, zh, c), device(x, zl, y, 1 - zh, c)
    c_flip = device(x, zl, y, zh, 1 - c)
    rows_x = (y % 2) * 2 + zh
    rows_d = (x - rows_x + 4) % 4
    rows_y = ((y // 2 + zl) % 2) * 2 + rows_d // 2
    rows_dev = device(rows_x, zl, rows_y, rows_d % 2, c)
    turn_dev = device(x, zl, rows_y, rows_d % 2, c)
    back_d = (y % 2) * 2 + zh
    back_dev = device((x + back_d) % 4, zl, ((y // 2 + zl) % 2) * 2 + x // 2, x % 2, c)
    moves = jnp.logical_or(rows_dev[0] != fi, rows_dev[1] != ti)
    turn_x = (x - back_d + 4) % 4
    turn_src = device(x, zl, ((y // 2 + zl) % 2) * 2 + turn_x // 2, turn_x % 2, c)
    turns = turn_dev[1] != ti
    shift_dev = device(turn_x, zl, y, zh, c)
    shifts = back_d != 0

    def local(n, src, dst):
        here = pltpu.make_async_copy(src, dst, local_sems.at[n])
        here.start()
        return here

    ref_here = [local(3, gate_r_in, gates.at[0]), local(4, up_r_in, gates.at[1])]
    depth = wpol_t_in.shape[1]
    pol_here = [local(5, gate_p_in, gates.at[2]), local(6, up_p_in, gates.at[3])]
    own = [
        local(7, mod_in, mods.at[0]),
        local(8, wref_in, wr.at[0]),
        local(9, wpol_t_in, wp.at[0, :, pl.ds(0, depth)]),
        local(10, wpol_i_in, wp.at[0, :, pl.ds(depth, depth)]),
    ]

    barrier = pltpu.get_barrier_semaphore()
    for dev in (x_up, x_down, x_opp, y_up, y_down, zl_flip, zh_flip, c_flip):
        pl.semaphore_signal(barrier, inc=1, device_id=dev, device_id_type=MESH)

    @pl.when(moves)
    def _():
        for dev in (rows_dev, back_dev):
            pl.semaphore_signal(barrier, inc=1, device_id=dev, device_id_type=MESH)

    @pl.when(turns)
    def _():
        for dev in (turn_dev, turn_src):
            pl.semaphore_signal(barrier, inc=1, device_id=dev, device_id_type=MESH)

    def hidden(first, out):
        def chunk(n):
            where = pl.ds(pl.multiple_of(n * 16, 16), 16)
            gate, up = gates[first, where].astype(f32), gates[first + 1, where].astype(f32)
            out[0, where] = (gate * jax.nn.sigmoid(gate) * up).astype(bf16)

        loop(ff // 16, chunk)

    for here in ref_here:
        here.wait()
    hidden(0, hr)
    pl.semaphore_wait(barrier, 8 + jnp.where(moves, 2, 0) + jnp.where(turns, 2, 0))

    started = []

    def copy(src, dst, dev):
        n = len(started)
        rdma = pltpu.make_async_remote_copy(
            src_ref=src,
            dst_ref=dst,
            send_sem=send_sems.at[n],
            recv_sem=recv_sems.at[n],
            device_id=dev,
            device_id_type=MESH,
        )
        started.append(rdma)
        rdma.start()
        return rdma

    def copy_or_stay(n, src, dst, dev, moves):
        rdma = pltpu.make_async_remote_copy(
            src_ref=src,
            dst_ref=dst,
            send_sem=send_sems.at[n],
            recv_sem=recv_sems.at[n],
            device_id=dev,
            device_id_type=MESH,
        )
        here = pltpu.make_async_copy(src, dst, local_sems.at[n - N_SEM])
        stays = jnp.logical_not(moves)

        @pl.when(moves)
        def _():
            rdma.start()

        @pl.when(stays)
        def _():
            here.start()

        def wait():
            @pl.when(moves)
            def _():
                rdma.wait()

            @pl.when(stays)
            def _():
                here.wait()

        return wait

    below, above, opp = (y + 3) % 4, (y + 1) % 4, (y + 2) % 4
    lo, hi = pl.ds(0, cut), pl.ds(cut, ff - cut)
    k_own = y * 2 + zh
    wait_turned = copy_or_stay(N_SEM, cot_in, turned, turn_dev, turns)
    m_up = copy(mod_in, mods.at[3], x_up)
    m_down = copy(mod_in, mods.at[1], x_down)
    m_opp = copy(mod_in, mods.at[2], x_opp)

    def spread_first(h):
        return copy(h.at[0, lo], h.at[3, lo], x_up), copy(h.at[0, hi], h.at[1, hi], x_down)

    def spread_last(h):
        return copy(h.at[0, hi], h.at[3, hi], x_up), copy(h.at[0, lo], h.at[1, lo], x_down)

    def pass_on(h, up_first, down_first):
        up_first.wait_recv()
        down_first.wait_recv()
        return copy(h.at[3, lo], h.at[2, lo], x_up), copy(h.at[1, hi], h.at[2, hi], x_down)

    h_up, h_down = spread_first(hr)
    some = wref_in.shape[0] // 4
    w_far = []

    def send_w(first, count):
        where = pl.ds(first * some, count * some)
        w_far.append(copy(wref_in.at[where], wr.at[1, where], zl_flip))

    send_w(0, 2)
    for here in pol_here:
        here.wait()
    hidden(2, hp)

    wait_turned()
    wait_moved = copy_or_stay(N_SEM + 2, turned, cr.at[c, k_own], shift_dev, shifts)
    h_up2, h_down2 = spread_last(hr)
    h_opp_lo, h_opp_hi = pass_on(hr, h_up, h_down)
    p_up, p_down = spread_first(hp)
    p_up2, p_down2 = spread_last(hp)
    wait_moved()
    cot_zh = [copy(cr.at[c, k_own], cr.at[c, k_own], zh_flip)]
    send_w(2, 1)
    for here in own:
        here.wait()
    send_w(3, 1)
    wp_far = [
        copy(wpol_t_in, wp.at[1, :, pl.ds(0, depth)], zl_flip),
        copy(wpol_i_in, wp.at[1, :, pl.ds(depth, depth)], zl_flip),
    ]
    for got in cot_zh:
        got.wait_recv()
    pair = cr.at[c, pl.ds(y * 2, 2)]
    cot_up = copy(pair, pair, y_up)
    cot_down = copy(pair, pair, y_down)
    cot_c = [copy(pair, pair, c_flip)]
    m_up.wait_recv()
    m_down.wait_recv()
    m_opp.wait_recv()
    h_up2.wait_recv()
    h_down2.wait_recv()

    def image(d, row, where):
        return mods[d, pl.ds(row, 1), where].astype(bf16)

    def ref_piece(d, slot):
        def tile(n):
            where = lanes(n)
            img = image(d, 0, where)
            block = hr[d, :, where]
            hs[pl.ds(0, ff)] = block * (1 - img)
            hs[pl.ds(ff, ff)] = block * img
            for r in range(2):
                there = pl.ds(pl.multiple_of((1 - c) * cols, cols), cols)
                away = jnp.dot(wr[r, there], hs[...], preferred_element_type=f32)
                aw[d, r, :, where] = away.astype(bf16)
                stay = pl.ds(pl.multiple_of(c * cols, cols), cols)
                kp[slot, r, :, where] = jnp.dot(wr[r, stay], hs[...], preferred_element_type=f32)

        loop(tiles, tile)
        return copy(aw.at[d], ar.at[d], c_flip)

    def ref_sum(d, slot, got):
        got.wait_recv()

        def tile(n):
            where = lanes(n)
            for r in range(2):
                total = kp[slot, r, :, where] + ar[d, r, :, where].astype(f32)
                sr[r * 4 + d, :, where] = total.astype(bf16)

        loop(tiles, tile)

    for got in w_far:
        got.wait_recv()
    got0 = ref_piece(0, 0)
    p_opp_lo, p_opp_hi = pass_on(hp, p_up, p_down)
    got1 = ref_piece(1, 1)
    ref_sum(0, 0, got0)
    got3 = ref_piece(3, 0)
    ref_sum(1, 1, got1)
    cot_up.wait_recv()
    cot_down.wait_recv()
    cot_opp_lo = copy(cr.at[c, below * 2], cr.at[c, below * 2], y_up)
    cot_opp_hi = copy(cr.at[c, above * 2 + 1], cr.at[c, above * 2 + 1], y_down)
    for at in (below, above):
        other = cr.at[c, pl.ds(at * 2, 2)]
        cot_c.append(copy(other, other, c_flip))
    h_opp_lo.wait_recv()
    h_opp_hi.wait_recv()
    got2 = ref_piece(2, 1)
    ref_sum(3, 0, got3)
    ref_sum(2, 1, got2)

    via_up = copy(sr.at[opp * 2], va, y_up)
    via_down = copy(sr.at[opp * 2 + 1], vb, y_down)
    first_up = copy(sr.at[above * 2 + 1], ga.at[1], y_up)
    first_down = copy(sr.at[below * 2], gb.at[0], y_down)

    cot_opp_lo.wait_recv()
    cot_opp_hi.wait_recv()
    other = cr.at[c, pl.ds(opp * 2, 2)]
    cot_c.append(copy(other, other, c_flip))

    def d_piece(d, store):
        def tile(n):
            where = lanes(n)
            img = image(d, 1, where)
            for r in range(2):
                for core in range(2):
                    block = cr[core, r * 4 + d, :, where]
                    at = r * 4 * cols + core * cols
                    cs[pl.ds(at, cols)] = block * (1 - img)
                    cs[pl.ds(at + 2 * cols, cols)] = block * img
            part = jnp.dot(wp[0], cs[pl.ds(0, 4 * cols)], preferred_element_type=f32)
            part += jnp.dot(wp[1], cs[pl.ds(4 * cols, 4 * cols)], preferred_element_type=f32)
            store(where, part)

        loop(tiles, tile)

    def store_dh(slot):
        def store(where, part):
            dh[slot, :, where] = part.astype(bf16)

        return store

    def down(r, core, modality):
        total = None
        for d in range(4):
            img = image(d, 1, slice(None))
            block = cr[core, r * 4 + d] * (img if modality else 1 - img)
            part = lax.dot_general(
                hp[d], block, (((1,), (1,)), ((), ())), preferred_element_type=f32
            )
            total = part if total is None else total + part
        return total

    def away(modality):
        def column(core):
            dws[modality, :, lanes(core)] = down(1, core, modality).astype(bf16)

        loop(2, column)

    for got in cot_c:
        got.wait_recv()
    for got in wp_far:
        got.wait_recv()
    d_piece(2, store_dh(2))
    d_via_up = copy(dh.at[2, lo], xa_via, x_up)
    d_via_down = copy(dh.at[2, hi], xb_via, x_down)
    p_up2.wait_recv()
    p_down2.wait_recv()
    p_opp_lo.wait_recv()
    p_opp_hi.wait_recv()
    away(0)
    dw_sent = [copy(dws.at[0], dwr.at[0], zl_flip)]
    via_up.wait_recv()
    via_down.wait_recv()

    def add_via(n):
        where = lanes(n)
        for at, via in ((above * 2, va), (below * 2 + 1, vb)):
            total = sr[at, :, where].astype(f32) + via[:, where].astype(f32)
            sr[at, :, where] = total.astype(bf16)

    loop(tiles, add_via)
    last_up = copy(sr.at[above * 2], ga.at[0], y_up)
    last_down = copy(sr.at[below * 2 + 1], gb.at[1], y_down)

    d_piece(1, store_dh(0))
    d_first_up = copy(dh.at[0, hi], xa.at[hi], x_up)
    d_piece(3, store_dh(1))
    d_first_down = copy(dh.at[1, lo], xb.at[lo], x_down)

    first_up.wait_recv()
    first_down.wait_recv()
    last_up.wait_recv()
    last_down.wait_recv()

    def y_sum(k, where):
        total = sr[y * 2 + k, :, where].astype(f32) + ga[k, :, where].astype(f32)
        return total + gb[k, :, where].astype(f32)

    def z_away(n):
        where = lanes(n)
        za[:, where] = y_sum(1 - zh, where).astype(bf16)

    loop(tiles, z_away)
    z_copy = [copy(za, zr, zh_flip)]
    away(1)

    d_via_up.wait_recv()
    d_via_down.wait_recv()

    def add_d(n):
        where = lanes(n)
        dh[0, lo, where] = (dh[0, lo, where].astype(f32) + xa_via[:, where].astype(f32)).astype(bf16)
        dh[1, hi, where] = (dh[1, hi, where].astype(f32) + xb_via[:, where].astype(f32)).astype(bf16)

    loop(tiles, add_d)
    d_last_up = copy(dh.at[0, lo], xa.at[lo], x_up)
    d_last_down = copy(dh.at[1, hi], xb.at[hi], x_down)
    dw_sent.append(copy(dws.at[1], dwr.at[1], zl_flip))

    def store_own(where, part):
        d_own[:, where] = part


    d_piece(0, store_own)
    for got in z_copy:
        got.wait_recv()

    def z_sum(n):
        where = lanes(n)
        fo[:, where] = (y_sum(zh, where) + zr[:, where].astype(f32)).astype(bf16)

    loop(tiles, z_sum)
    wait_back = copy_or_stay(N_SEM + 1, fo, out_ref, back_dev, moves)

    for modality, out in enumerate((out_t, out_i)):

        def column(core, modality=modality, out=out):
            out[:, lanes(core)] = down(0, core, modality)

        loop(2, column)

    for got in (d_first_up, d_first_down, d_last_up, d_last_down):
        got.wait_recv()

    def d_sum(n):
        where = pl.ds(pl.multiple_of(n * 16, 16), 16)
        gate, up = gates[2, where].astype(f32), gates[3, where].astype(f32)
        d_hidden = d_own[where] + xa[where].astype(f32) + xb[where].astype(f32)
        sig = jax.nn.sigmoid(gate)
        out_gate[where] = (d_hidden * up * sig * (1.0 + gate * (1.0 - sig))).astype(bf16)
        out_up[where] = (d_hidden * (gate * sig)).astype(bf16)

    loop(ff // 16, d_sum)
    for modality, out in enumerate((out_t, out_i)):
        dw_sent[modality].wait_recv()

        def dw_sum(core, modality=modality, out=out):
            where = lanes(core)
            out[:, where] = out[:, where] + dwr[modality, :, where].astype(f32)

        loop(2, dw_sum)
    wait_back()
    for rdma in started:
        rdma.wait_send()


def communicate(cot, mod, gate_r, up_r, gate_p, up_p, wref, wpol_t, wpol_i):
    ff, rows = gate_r.shape
    cols = cot.shape[0]
    depth = wref.shape[0]
    cut = (ff // 32) * 16
    vmem = pltpu.VMEM
    scratch = [
        vmem((4, ff, rows), bf16),
        vmem((cols, rows), bf16),
        vmem((ff, rows), f32),
        vmem((4, ff, rows), bf16),
        vmem((4, ff, rows), bf16),
        vmem((2, depth, 2 * ff), bf16),
        vmem((2, ff, 2 * depth), bf16),
        vmem((2, 8, cols, rows), bf16),
        vmem((4, 8, rows), f32),
        vmem((2 * ff, 256), bf16),
        vmem((8 * cols, 256), bf16),
        vmem((4, 2, cols, rows), bf16),
        vmem((4, 2, cols, rows), bf16),
        vmem((2, 2, cols, rows), f32),
        vmem((8, cols, rows), bf16),
        vmem((cols, rows), bf16),
        vmem((cols, rows), bf16),
        vmem((2, cols, rows), bf16),
        vmem((2, cols, rows), bf16),
        vmem((cols, rows), bf16),
        vmem((cols, rows), bf16),
        vmem((cols, rows), bf16),
        vmem((3, ff, rows), bf16),
        vmem((cut, rows), bf16),
        vmem((ff - cut, rows), bf16),
        vmem((ff, rows), bf16),
        vmem((ff, rows), bf16),
        vmem((2, ff, depth), bf16),
        vmem((2, ff, depth), bf16),
        pltpu.SemaphoreType.DMA((N_SEM + 3,)),
        pltpu.SemaphoreType.DMA((N_SEM + 3,)),
        pltpu.SemaphoreType.DMA((11,)),
    ]
    anywhere = pl.BlockSpec(memory_space=pl.ANY)
    in_vmem = pl.BlockSpec(memory_space=vmem)
    return pl.pallas_call(
        step_kernel,
        out_shape=(
            jax.ShapeDtypeStruct((cols, rows), bf16),
            jax.ShapeDtypeStruct((ff, rows), bf16),
            jax.ShapeDtypeStruct((ff, rows), bf16),
            jax.ShapeDtypeStruct((ff, depth), f32),
            jax.ShapeDtypeStruct((ff, depth), f32),
        ),
        in_specs=[anywhere] * 9,
        out_specs=(in_vmem,) * 5,
        scratch_shapes=scratch,
        compiler_params=pltpu.CompilerParams(
            collective_id=0, has_side_effects=True, vmem_limit_bytes=66_000_000
        ),
    )(cot, mod, gate_r, up_r, gate_p, up_p, wref, wpol_t, wpol_i)


def per_device(
    ref_gate,
    ref_up,
    ref_residual,
    ref_modality,
    ref_down_text,
    ref_down_image,
    pol_gate,
    pol_up,
    pol_modality,
    pol_segment,
    pair_margin,
    token_cotangent,
    pol_down_text,
    pol_down_image,
):
    rows = ref_gate.shape[0]
    seg_ids = jnp.arange(2 * pair_margin.shape[0], dtype=jnp.int32)
    pair_weight = dpo_beta * jax.nn.sigmoid(-dpo_beta * pair_margin)
    table = jnp.repeat(pair_weight, 2) * jnp.where(seg_ids % 2 == 0, -1.0, 1.0).astype(f32)
    coef = jnp.sum(
        jnp.where(pol_segment[None, :] == seg_ids[:, None], table[:, None], f32(0.0)), axis=0
    )
    cot = (coef[None, :] * token_cotangent.T.astype(f32)).astype(bf16)
    mod = jnp.stack([ref_modality == 1, pol_modality == 1]).astype(f32)
    mod = jnp.concatenate([mod, jnp.zeros((6, rows), f32)], axis=0)

    w_ref = jnp.concatenate([ref_down_text, ref_down_image], axis=1)
    summed, grad_gate, grad_up, grad_t, grad_i = communicate(
        cot,
        mod,
        ref_gate.T,
        ref_up.T,
        pol_gate.T,
        pol_up.T,
        w_ref,
        pol_down_text.T,
        pol_down_image.T,
    )
    ref_out = (summed.T.astype(f32) + ref_residual.astype(f32)).astype(bf16)
    return (ref_out, grad_gate.T, grad_up.T, grad_t.T, grad_i.T)


def solution(mesh):
    spec = P("fsdp", "tp")
    in_specs = (
        spec,
        spec,
        spec,
        P("fsdp"),
        spec,
        spec,
        spec,
        spec,
        P("fsdp"),
        P("fsdp"),
        P(),
        spec,
        spec,
        spec,
    )
    return jax.shard_map(
        per_device, mesh=mesh, in_specs=in_specs, out_specs=(spec,) * 5, check_vma=False
    )
```

```python
import jax
import jax.numpy as jnp
from jax import lax
from jax.experimental import pallas as pl
from jax.experimental.pallas import tpu as pltpu
from jax.sharding import PartitionSpec as P

dpo_beta = 0.1
bf16 = jnp.bfloat16
f32 = jnp.float32
MESH = pl.DeviceIdType.MESH


N_SEM = 64


def lanes(n, width=256):
    return pl.ds(pl.multiple_of(n * width, width), width)


def loop(count, body):
    def step(n, carry):
        body(n)
        return carry

    lax.fori_loop(0, count, step, 0)


def step_kernel(
    token_in,
    ref_mod_in,
    pol_mod_in,
    segment_in,
    margin_in,
    gate_r_in,
    up_r_in,
    gate_p_in,
    up_p_in,
    wref_t_in,
    wref_i_in,
    wpol_t_in,
    wpol_i_in,
    out_ref,
    out_gate,
    out_up,
    own_t,
    own_i,
    far_t,
    far_i,
    dwo,
    gates,
    turned,
    tokens,
    cot_in,
    mod_in,
    d_own,
    hr,
    hp,
    wrt,
    wr,
    wp,
    cr,
    mods,
    hs,
    cs,
    aw,
    ar,
    kp,
    sr,
    va,
    vb,
    ga,
    gb,
    za,
    zr,
    fo,
    dh,
    xa_via,
    xb_via,
    xa,
    xb,
    dws,
    send_sems,
    recv_sems,
    local_sems,
):
    fi = lax.axis_index("fsdp")
    ti = lax.axis_index("tp")
    zl, x = fi // 4, fi % 4
    y, zh, c = ti // 4, (ti // 2) % 2, ti % 2
    ff, rows = gate_r_in.shape
    cols = token_in.shape[1]
    cut = (ff // 32) * 16
    tiles = rows // 256

    def device(x2, zl2, y2, zh2, c2):
        return (zl2 * 4 + x2, y2 * 4 + zh2 * 2 + c2)

    x_up, x_down = device((x + 1) % 4, zl, y, zh, c), device((x + 3) % 4, zl, y, zh, c)
    x_opp = device((x + 2) % 4, zl, y, zh, c)
    y_up, y_down = device(x, zl, (y + 1) % 4, zh, c), device(x, zl, (y + 3) % 4, zh, c)
    zl_flip, zh_flip = device(x, 1 - zl, y, zh, c), device(x, zl, y, 1 - zh, c)
    c_flip = device(x, zl, y, zh, 1 - c)
    rows_x = (y % 2) * 2 + zh
    rows_d = (x - rows_x + 4) % 4
    rows_y = ((y // 2 + zl) % 2) * 2 + rows_d // 2
    rows_dev = device(rows_x, zl, rows_y, rows_d % 2, c)
    turn_dev = device(x, zl, rows_y, rows_d % 2, c)
    back_d = (y % 2) * 2 + zh
    back_dev = device((x + back_d) % 4, zl, ((y // 2 + zl) % 2) * 2 + x // 2, x % 2, c)
    moves = jnp.logical_or(rows_dev[0] != fi, rows_dev[1] != ti)
    turn_x = (x - back_d + 4) % 4
    turn_src = device(x, zl, ((y // 2 + zl) % 2) * 2 + turn_x // 2, turn_x % 2, c)
    turns = turn_dev[1] != ti
    shift_dev = device(turn_x, zl, y, zh, c)
    shifts = back_d != 0

    def local(n, src, dst):
        here = pltpu.make_async_copy(src, dst, local_sems.at[n])
        here.start()
        return here

    token_here = local(15, token_in, tokens)
    ref_here = [local(3, gate_r_in, gates.at[0]), local(4, up_r_in, gates.at[1])]
    depth = wpol_t_in.shape[1]
    pol_here = [local(5, gate_p_in, gates.at[2]), local(6, up_p_in, gates.at[3])]
    own = [
        local(8, wref_t_in, wrt.at[0, 0]),
        local(16, wref_i_in, wrt.at[0, 1]),
        local(9, wpol_t_in, wp.at[0, :, pl.ds(0, depth)]),
        local(10, wpol_i_in, wp.at[0, :, pl.ds(depth, depth)]),
    ]

    barrier = pltpu.get_barrier_semaphore()
    for dev in (x_up, x_down, x_opp, y_up, y_down, zl_flip, zh_flip, c_flip):
        pl.semaphore_signal(barrier, inc=1, device_id=dev, device_id_type=MESH)

    @pl.when(moves)
    def _():
        for dev in (rows_dev, back_dev):
            pl.semaphore_signal(barrier, inc=1, device_id=dev, device_id_type=MESH)

    @pl.when(turns)
    def _():
        for dev in (turn_dev, turn_src):
            pl.semaphore_signal(barrier, inc=1, device_id=dev, device_id_type=MESH)

    def hidden(first, out):
        def chunk(n):
            where = pl.ds(pl.multiple_of(n * 16, 16), 16)
            gate, up = gates[first, where].astype(f32), gates[first + 1, where].astype(f32)
            out[0, where] = (gate * jax.nn.sigmoid(gate) * up).astype(bf16)

        loop(ff // 16, chunk)

    segment = segment_in[...].reshape(1, rows)
    coef = jnp.zeros((1, rows), f32)
    for p in range(margin_in.shape[0]):
        margin = jnp.full((1, rows), margin_in[p], f32)
        weight = dpo_beta * jax.nn.sigmoid(-dpo_beta * margin)
        coef = jnp.where(segment == 2 * p, -weight, coef)
        coef = jnp.where(segment == 2 * p + 1, weight, coef)
    images = [(m[...].reshape(1, rows) == 1).astype(f32) for m in (ref_mod_in, pol_mod_in)]
    for where in (mod_in, mods.at[0]):
        for row, value in enumerate((*images, coef)):
            where[pl.ds(row, 1)] = value
        where[pl.ds(3, 5)] = jnp.zeros((5, rows), f32)
    token_here.wait()

    def weigh(n):
        where = lanes(n)
        turned_block = tokens[where, :].astype(f32).T
        cot_in[:, where] = (turned_block * mods[0, pl.ds(2, 1), where]).astype(bf16)

    loop(tiles, weigh)
    for here in ref_here:
        here.wait()
    hidden(0, hr)
    pl.semaphore_wait(barrier, 8 + jnp.where(moves, 2, 0) + jnp.where(turns, 2, 0))

    started = []

    def copy(src, dst, dev):
        n = len(started)
        rdma = pltpu.make_async_remote_copy(
            src_ref=src,
            dst_ref=dst,
            send_sem=send_sems.at[n],
            recv_sem=recv_sems.at[n],
            device_id=dev,
            device_id_type=MESH,
        )
        started.append(rdma)
        rdma.start()
        return rdma

    def copy_or_stay(n, src, dst, dev, moves):
        rdma = pltpu.make_async_remote_copy(
            src_ref=src,
            dst_ref=dst,
            send_sem=send_sems.at[n],
            recv_sem=recv_sems.at[n],
            device_id=dev,
            device_id_type=MESH,
        )
        here = pltpu.make_async_copy(src, dst, local_sems.at[n - N_SEM])
        stays = jnp.logical_not(moves)

        @pl.when(moves)
        def _():
            rdma.start()

        @pl.when(stays)
        def _():
            here.start()

        def wait():
            @pl.when(moves)
            def _():
                rdma.wait()

            @pl.when(stays)
            def _():
                here.wait()

        return wait

    below, above, opp = (y + 3) % 4, (y + 1) % 4, (y + 2) % 4
    lo, hi = pl.ds(0, cut), pl.ds(cut, ff - cut)
    k_own = y * 2 + zh
    wait_turned = copy_or_stay(N_SEM, cot_in, turned, turn_dev, turns)
    m_up = copy(mod_in, mods.at[3], x_up)
    m_down = copy(mod_in, mods.at[1], x_down)
    m_opp = copy(mod_in, mods.at[2], x_opp)

    def spread_first(h):
        return copy(h.at[0, lo], h.at[3, lo], x_up), copy(h.at[0, hi], h.at[1, hi], x_down)

    def spread_last(h):
        return copy(h.at[0, hi], h.at[3, hi], x_up), copy(h.at[0, lo], h.at[1, lo], x_down)

    def pass_on(h, up_first, down_first):
        up_first.wait_recv()
        down_first.wait_recv()
        return copy(h.at[3, lo], h.at[2, lo], x_up), copy(h.at[1, hi], h.at[2, hi], x_down)

    h_up, h_down = spread_first(hr)
    w_far = []

    def send_w(modality, src, where):
        w_far.append(copy(src.at[where], wrt.at[1, modality, where], zl_flip))

    def flip(r, modality):
        for first in range(0, ff, 128):
            count = min(128, ff - first)
            block = wrt[r, modality, pl.ds(first, count), :]
            wr[r, modality, :, pl.ds(first, count)] = block.T

    send_w(0, wref_t_in, pl.ds(0, ff))
    for here in pol_here:
        here.wait()
    hidden(2, hp)
    for here in own:
        here.wait()
    flip(0, 0)
    flip(0, 1)

    wait_turned()
    wait_moved = copy_or_stay(N_SEM + 2, turned, cr.at[c, k_own], shift_dev, shifts)
    h_up2, h_down2 = spread_last(hr)
    h_opp_lo, h_opp_hi = pass_on(hr, h_up, h_down)
    p_up, p_down = spread_first(hp)
    p_up2, p_down2 = spread_last(hp)
    wait_moved()
    cot_zh = [copy(cr.at[c, k_own], cr.at[c, k_own], zh_flip)]
    send_w(1, wref_i_in, lo)
    send_w(1, wref_i_in, hi)
    wp_far = [
        copy(wpol_t_in, wp.at[1, :, pl.ds(0, depth)], zl_flip),
        copy(wpol_i_in, wp.at[1, :, pl.ds(depth, depth)], zl_flip),
    ]
    for got in cot_zh:
        got.wait_recv()
    pair = cr.at[c, pl.ds(y * 2, 2)]
    cot_up = copy(pair, pair, y_up)
    cot_down = copy(pair, pair, y_down)
    cot_c = [copy(pair, pair, c_flip)]
    m_up.wait_recv()
    m_down.wait_recv()
    m_opp.wait_recv()
    h_up2.wait_recv()
    h_down2.wait_recv()

    def image(d, row, where):
        return mods[d, pl.ds(row, 1), where].astype(bf16)

    def ref_piece(d, slot):
        def tile(n):
            where = lanes(n)
            img = image(d, 0, where)
            block = hr[d, :, where]
            hs[0] = block * (1 - img)
            hs[1] = block * img
            for r in range(2):
                there = pl.ds(pl.multiple_of((1 - c) * cols, cols), cols)
                away = jnp.dot(wr[r, 0, there], hs[0], preferred_element_type=f32)
                away += jnp.dot(wr[r, 1, there], hs[1], preferred_element_type=f32)
                aw[d, r, :, where] = away.astype(bf16)
                stay = pl.ds(pl.multiple_of(c * cols, cols), cols)
                kept = jnp.dot(wr[r, 0, stay], hs[0], preferred_element_type=f32)
                kept += jnp.dot(wr[r, 1, stay], hs[1], preferred_element_type=f32)
                kp[slot, r, :, where] = kept

        loop(tiles, tile)
        return copy(aw.at[d], ar.at[d], c_flip)

    def ref_sum(d, slot, got):
        got.wait_recv()

        def tile(n):
            where = lanes(n)
            for r in range(2):
                total = kp[slot, r, :, where] + ar[d, r, :, where].astype(f32)
                sr[r * 4 + d, :, where] = total.astype(bf16)

        loop(tiles, tile)

    w_far[0].wait_recv()
    flip(1, 0)
    w_far[1].wait_recv()
    w_far[2].wait_recv()
    flip(1, 1)
    got0 = ref_piece(0, 0)
    p_opp_lo, p_opp_hi = pass_on(hp, p_up, p_down)
    got1 = ref_piece(1, 1)
    ref_sum(0, 0, got0)
    got3 = ref_piece(3, 0)
    ref_sum(1, 1, got1)
    cot_up.wait_recv()
    cot_down.wait_recv()
    cot_opp_lo = copy(cr.at[c, below * 2], cr.at[c, below * 2], y_up)
    cot_opp_hi = copy(cr.at[c, above * 2 + 1], cr.at[c, above * 2 + 1], y_down)
    for at in (below, above):
        other = cr.at[c, pl.ds(at * 2, 2)]
        cot_c.append(copy(other, other, c_flip))
    h_opp_lo.wait_recv()
    h_opp_hi.wait_recv()
    got2 = ref_piece(2, 1)
    ref_sum(3, 0, got3)
    ref_sum(2, 1, got2)

    via_up = copy(sr.at[opp * 2], va, y_up)
    via_down = copy(sr.at[opp * 2 + 1], vb, y_down)
    first_up = copy(sr.at[above * 2 + 1], ga.at[1], y_up)
    first_down = copy(sr.at[below * 2], gb.at[0], y_down)

    cot_opp_lo.wait_recv()
    cot_opp_hi.wait_recv()
    other = cr.at[c, pl.ds(opp * 2, 2)]
    cot_c.append(copy(other, other, c_flip))

    def d_piece(d, store):
        def tile(n):
            where = lanes(n)
            img = image(d, 1, where)
            for r in range(2):
                for core in range(2):
                    block = cr[core, r * 4 + d, :, where]
                    at = r * 4 * cols + core * cols
                    cs[pl.ds(at, cols)] = block * (1 - img)
                    cs[pl.ds(at + 2 * cols, cols)] = block * img
            part = jnp.dot(wp[0], cs[pl.ds(0, 4 * cols)], preferred_element_type=f32)
            part += jnp.dot(wp[1], cs[pl.ds(4 * cols, 4 * cols)], preferred_element_type=f32)
            store(where, part)

        loop(tiles, tile)

    def store_dh(slot):
        def store(where, part):
            dh[slot, :, where] = part.astype(bf16)

        return store

    def down(r, core, modality):
        total = None
        for d in range(4):
            img = image(d, 1, slice(None))
            block = cr[core, r * 4 + d] * (img if modality else 1 - img)
            part = lax.dot_general(
                hp[d], block, (((1,), (1,)), ((), ())), preferred_element_type=f32
            )
            total = part if total is None else total + part
        return total

    def away(modality):
        def column(core):
            dws[modality, :, lanes(core)] = down(1, core, modality).astype(bf16)

        loop(2, column)

    for got in cot_c:
        got.wait_recv()
    p_up2.wait_recv()
    p_down2.wait_recv()
    p_opp_lo.wait_recv()
    p_opp_hi.wait_recv()
    away(0)
    dw_sent = [copy(dws.at[0], far_t, zl_flip)]
    for got in wp_far:
        got.wait_recv()
    d_piece(2, store_dh(2))
    d_via_up = copy(dh.at[2, lo], xa_via, x_up)
    d_via_down = copy(dh.at[2, hi], xb_via, x_down)
    via_up.wait_recv()
    via_down.wait_recv()

    def add_via(n):
        where = lanes(n)
        for at, via in ((above * 2, va), (below * 2 + 1, vb)):
            total = sr[at, :, where].astype(f32) + via[:, where].astype(f32)
            sr[at, :, where] = total.astype(bf16)

    loop(tiles, add_via)
    last_up = copy(sr.at[above * 2], ga.at[0], y_up)
    last_down = copy(sr.at[below * 2 + 1], gb.at[1], y_down)

    d_piece(1, store_dh(0))
    d_first_up = copy(dh.at[0, hi], xa.at[hi], x_up)
    d_piece(3, store_dh(1))
    d_first_down = copy(dh.at[1, lo], xb.at[lo], x_down)

    first_up.wait_recv()
    first_down.wait_recv()
    last_up.wait_recv()
    last_down.wait_recv()

    def y_sum(k, where):
        total = sr[y * 2 + k, :, where].astype(f32) + ga[k, :, where].astype(f32)
        return total + gb[k, :, where].astype(f32)

    def z_away(n):
        where = lanes(n)
        za[:, where] = y_sum(1 - zh, where).astype(bf16)

    loop(tiles, z_away)
    z_copy = [copy(za, zr, zh_flip)]
    away(1)

    d_via_up.wait_recv()
    d_via_down.wait_recv()

    def add_d(n):
        where = lanes(n)
        dh[0, lo, where] = (dh[0, lo, where].astype(f32) + xa_via[:, where].astype(f32)).astype(bf16)
        dh[1, hi, where] = (dh[1, hi, where].astype(f32) + xb_via[:, where].astype(f32)).astype(bf16)

    loop(tiles, add_d)
    d_last_up = copy(dh.at[0, lo], xa.at[lo], x_up)
    d_last_down = copy(dh.at[1, hi], xb.at[hi], x_down)
    dw_sent.append(copy(dws.at[1], far_i, zl_flip))

    def store_own(where, part):
        d_own[:, where] = part


    d_piece(0, store_own)
    for got in z_copy:
        got.wait_recv()

    def z_sum(n):
        where = lanes(n)
        fo[where, :] = (y_sum(zh, where) + zr[:, where].astype(f32)).T.astype(bf16)

    loop(tiles, z_sum)
    wait_back = copy_or_stay(N_SEM + 1, fo, out_ref, back_dev, moves)

    flushed = []
    for modality, out in enumerate((own_t, own_i)):

        def column(core, modality=modality):
            dwo[modality, :, lanes(core)] = down(0, core, modality)

        loop(2, column)
        flushed.append(local(11 + modality, dwo.at[modality], out))

    for got in (d_first_up, d_first_down, d_last_up, d_last_down):
        got.wait_recv()

    def d_sum(n):
        where = pl.ds(pl.multiple_of(n * 16, 16), 16)
        gate, up = gates[2, where].astype(f32), gates[3, where].astype(f32)
        d_hidden = d_own[where] + xa[where].astype(f32) + xb[where].astype(f32)
        sig = jax.nn.sigmoid(gate)
        gates[0, where] = (d_hidden * up * sig * (1.0 + gate * (1.0 - sig))).astype(bf16)
        gates[1, where] = (d_hidden * (gate * sig)).astype(bf16)

    loop(ff // 16, d_sum)
    flushed.append(local(13, gates.at[0], out_gate))
    flushed.append(local(14, gates.at[1], out_up))
    for got in dw_sent:
        got.wait_recv()
    for here in flushed:
        here.wait()
    wait_back()
    for rdma in started:
        rdma.wait_send()


def communicate(cot, ref_mod, pol_mod, segment, margin, gate_r, up_r, gate_p, up_p, wref_t, wref_i, wpol_t, wpol_i):
    ff, rows = gate_r.shape
    cols = cot.shape[1]
    depth = wref_t.shape[1]
    cut = (ff // 32) * 16
    vmem = pltpu.VMEM
    scratch = [
        vmem((2, ff, depth), f32),
        vmem((4, ff, rows), bf16),
        vmem((cols, rows), bf16),
        vmem((rows, cols), bf16),
        vmem((cols, rows), bf16),
        vmem((8, rows), f32),
        vmem((ff, rows), f32),
        vmem((4, ff, rows), bf16),
        vmem((4, ff, rows), bf16),
        vmem((2, 2, ff, depth), bf16),
        vmem((2, 2, depth, ff), bf16),
        vmem((2, ff, 2 * depth), bf16),
        vmem((2, 8, cols, rows), bf16),
        vmem((4, 8, rows), f32),
        vmem((2, ff, 256), bf16),
        vmem((8 * cols, 256), bf16),
        vmem((4, 2, cols, rows), bf16),
        vmem((4, 2, cols, rows), bf16),
        vmem((2, 2, cols, rows), f32),
        vmem((8, cols, rows), bf16),
        vmem((cols, rows), bf16),
        vmem((cols, rows), bf16),
        vmem((2, cols, rows), bf16),
        vmem((2, cols, rows), bf16),
        vmem((cols, rows), bf16),
        vmem((cols, rows), bf16),
        vmem((rows, cols), bf16),
        vmem((3, ff, rows), bf16),
        vmem((cut, rows), bf16),
        vmem((ff - cut, rows), bf16),
        vmem((ff, rows), bf16),
        vmem((ff, rows), bf16),
        vmem((2, ff, depth), bf16),
        pltpu.SemaphoreType.DMA((N_SEM + 3,)),
        pltpu.SemaphoreType.DMA((N_SEM + 3,)),
        pltpu.SemaphoreType.DMA((17,)),
    ]
    anywhere = pl.BlockSpec(memory_space=pl.ANY)
    return pl.pallas_call(
        step_kernel,
        out_shape=(
            jax.ShapeDtypeStruct((rows, cols), bf16),
            jax.ShapeDtypeStruct((ff, rows), bf16),
            jax.ShapeDtypeStruct((ff, rows), bf16),
            jax.ShapeDtypeStruct((ff, depth), f32),
            jax.ShapeDtypeStruct((ff, depth), f32),
            jax.ShapeDtypeStruct((ff, depth), bf16),
            jax.ShapeDtypeStruct((ff, depth), bf16),
        ),
        in_specs=[anywhere] + [pl.BlockSpec(memory_space=vmem)] * 3 + [pl.BlockSpec(memory_space=pltpu.SMEM)] + [anywhere] * 8,
        out_specs=(anywhere,) * 7,
        scratch_shapes=scratch,
        compiler_params=pltpu.CompilerParams(
            collective_id=0, has_side_effects=True, vmem_limit_bytes=66_000_000
        ),
    )(cot, ref_mod, pol_mod, segment, margin, gate_r, up_r, gate_p, up_p, wref_t, wref_i, wpol_t, wpol_i)


def per_device(
    ref_gate,
    ref_up,
    ref_residual,
    ref_modality,
    ref_down_text,
    ref_down_image,
    pol_gate,
    pol_up,
    pol_modality,
    pol_segment,
    pair_margin,
    token_cotangent,
    pol_down_text,
    pol_down_image,
):
    rows = ref_gate.shape[0]
    summed, grad_gate, grad_up, own_t, own_i, far_t, far_i = communicate(
        token_cotangent,
        ref_modality,
        pol_modality,
        pol_segment,
        pair_margin,
        ref_gate.T,
        ref_up.T,
        pol_gate.T,
        pol_up.T,
        ref_down_text.T,
        ref_down_image.T,
        pol_down_text.T,
        pol_down_image.T,
    )
    ref_out = (summed.astype(f32) + ref_residual.astype(f32)).astype(bf16)
    grad_t = own_t + far_t.astype(f32)
    grad_i = own_i + far_i.astype(f32)
    return (ref_out, grad_gate.T, grad_up.T, grad_t.T, grad_i.T)


def solution(mesh):
    spec = P("fsdp", "tp")
    in_specs = (
        spec,
        spec,
        spec,
        P("fsdp"),
        spec,
        spec,
        spec,
        spec,
        P("fsdp"),
        P("fsdp"),
        P(),
        spec,
        spec,
        spec,
    )
    return jax.shard_map(
        per_device, mesh=mesh, in_specs=in_specs, out_specs=(spec,) * 5, check_vma=False
    )
```

```python
import jax
import jax.numpy as jnp
from jax import lax
from jax.experimental import pallas as pl
from jax.experimental.pallas import tpu as pltpu
from jax.sharding import PartitionSpec as P

dpo_beta = 0.1
bf16 = jnp.bfloat16
f32 = jnp.float32
MESH = pl.DeviceIdType.MESH


N_SEM = 64


def lanes(n, width=256):
    return pl.ds(pl.multiple_of(n * width, width), width)


def loop(count, body):
    def step(n, carry):
        body(n)
        return carry

    lax.fori_loop(0, count, step, 0)


def step_kernel(
    token_in,
    residual_in,
    ref_mod_in,
    pol_mod_in,
    segment_in,
    margin_in,
    gate_r_in,
    up_r_in,
    gate_p_in,
    up_p_in,
    wref_t_in,
    wref_i_in,
    wpol_t_in,
    wpol_i_in,
    out_ref,
    out_gate,
    out_up,
    own_t,
    own_i,
    far_t,
    far_i,
    dwo,
    gates,
    turned,
    tokens,
    residual,
    landed,
    cot_in,
    mod_in,
    d_own,
    hr,
    hp,
    wrt,
    wr,
    wp,
    cr,
    mods,
    hs,
    cs,
    aw,
    ar,
    kp,
    sr,
    va,
    vb,
    ga,
    gb,
    za,
    zr,
    fo,
    dh,
    xa_via,
    xb_via,
    xa,
    xb,
    dws,
    send_sems,
    recv_sems,
    local_sems,
):
    fi = lax.axis_index("fsdp")
    ti = lax.axis_index("tp")
    zl, x = fi // 4, fi % 4
    y, zh, c = ti // 4, (ti // 2) % 2, ti % 2
    ff, rows = gate_r_in.shape
    cols = token_in.shape[1]
    cut = (ff // 32) * 16
    tiles = rows // 256

    def device(x2, zl2, y2, zh2, c2):
        return (zl2 * 4 + x2, y2 * 4 + zh2 * 2 + c2)

    x_up, x_down = device((x + 1) % 4, zl, y, zh, c), device((x + 3) % 4, zl, y, zh, c)
    x_opp = device((x + 2) % 4, zl, y, zh, c)
    y_up, y_down = device(x, zl, (y + 1) % 4, zh, c), device(x, zl, (y + 3) % 4, zh, c)
    zl_flip, zh_flip = device(x, 1 - zl, y, zh, c), device(x, zl, y, 1 - zh, c)
    c_flip = device(x, zl, y, zh, 1 - c)
    rows_x = (y % 2) * 2 + zh
    rows_d = (x - rows_x + 4) % 4
    rows_y = ((y // 2 + zl) % 2) * 2 + rows_d // 2
    rows_dev = device(rows_x, zl, rows_y, rows_d % 2, c)
    turn_dev = device(x, zl, rows_y, rows_d % 2, c)
    back_d = (y % 2) * 2 + zh
    back_dev = device((x + back_d) % 4, zl, ((y // 2 + zl) % 2) * 2 + x // 2, x % 2, c)
    moves = jnp.logical_or(rows_dev[0] != fi, rows_dev[1] != ti)
    turn_x = (x - back_d + 4) % 4
    turn_src = device(x, zl, ((y // 2 + zl) % 2) * 2 + turn_x // 2, turn_x % 2, c)
    turns = turn_dev[1] != ti
    shift_dev = device(turn_x, zl, y, zh, c)
    shifts = back_d != 0

    def local(n, src, dst):
        here = pltpu.make_async_copy(src, dst, local_sems.at[n])
        here.start()
        return here

    token_here = local(15, token_in, tokens)
    ref_here = [local(3, gate_r_in, gates.at[0]), local(4, up_r_in, gates.at[1])]
    depth = wpol_t_in.shape[1]
    pol_here = [local(5, gate_p_in, gates.at[2]), local(6, up_p_in, gates.at[3])]
    own = [
        local(17, residual_in, residual),
        local(8, wref_t_in, wrt.at[0, 0]),
        local(16, wref_i_in, wrt.at[0, 1]),
        local(9, wpol_t_in, wp.at[0, :, pl.ds(0, depth)]),
        local(10, wpol_i_in, wp.at[0, :, pl.ds(depth, depth)]),
    ]

    barrier = pltpu.get_barrier_semaphore()
    for dev in (x_up, x_down, x_opp, y_up, y_down, zl_flip, zh_flip, c_flip):
        pl.semaphore_signal(barrier, inc=1, device_id=dev, device_id_type=MESH)

    @pl.when(moves)
    def _():
        for dev in (rows_dev, back_dev):
            pl.semaphore_signal(barrier, inc=1, device_id=dev, device_id_type=MESH)

    @pl.when(turns)
    def _():
        for dev in (turn_dev, turn_src):
            pl.semaphore_signal(barrier, inc=1, device_id=dev, device_id_type=MESH)

    def hidden(first, out):
        def chunk(n):
            where = pl.ds(pl.multiple_of(n * 16, 16), 16)
            gate, up = gates[first, where].astype(f32), gates[first + 1, where].astype(f32)
            out[0, where] = (gate * jax.nn.sigmoid(gate) * up).astype(bf16)

        loop(ff // 16, chunk)

    segment = segment_in[...].reshape(1, rows)
    coef = jnp.zeros((1, rows), f32)
    for p in range(margin_in.shape[0]):
        margin = jnp.full((1, rows), margin_in[p], f32)
        weight = dpo_beta * jax.nn.sigmoid(-dpo_beta * margin)
        coef = jnp.where(segment == 2 * p, -weight, coef)
        coef = jnp.where(segment == 2 * p + 1, weight, coef)
    images = [(m[...].reshape(1, rows) == 1).astype(f32) for m in (ref_mod_in, pol_mod_in)]
    for where in (mod_in, mods.at[0]):
        for row, value in enumerate((*images, coef)):
            where[pl.ds(row, 1)] = value
        where[pl.ds(3, 5)] = jnp.zeros((5, rows), f32)
    token_here.wait()

    def weigh(n):
        where = lanes(n)
        turned_block = tokens[where, :].astype(f32).T
        cot_in[:, where] = (turned_block * mods[0, pl.ds(2, 1), where]).astype(bf16)

    loop(tiles, weigh)
    for here in ref_here:
        here.wait()
    hidden(0, hr)
    pl.semaphore_wait(barrier, 8 + jnp.where(moves, 2, 0) + jnp.where(turns, 2, 0))

    started = []

    def copy(src, dst, dev):
        n = len(started)
        rdma = pltpu.make_async_remote_copy(
            src_ref=src,
            dst_ref=dst,
            send_sem=send_sems.at[n],
            recv_sem=recv_sems.at[n],
            device_id=dev,
            device_id_type=MESH,
        )
        started.append(rdma)
        rdma.start()
        return rdma

    def copy_or_stay(n, src, dst, dev, moves):
        rdma = pltpu.make_async_remote_copy(
            src_ref=src,
            dst_ref=dst,
            send_sem=send_sems.at[n],
            recv_sem=recv_sems.at[n],
            device_id=dev,
            device_id_type=MESH,
        )
        here = pltpu.make_async_copy(src, dst, local_sems.at[n - N_SEM])
        stays = jnp.logical_not(moves)

        @pl.when(moves)
        def _():
            rdma.start()

        @pl.when(stays)
        def _():
            here.start()

        def wait():
            @pl.when(moves)
            def _():
                rdma.wait()

            @pl.when(stays)
            def _():
                here.wait()

        return wait

    below, above, opp = (y + 3) % 4, (y + 1) % 4, (y + 2) % 4
    lo, hi = pl.ds(0, cut), pl.ds(cut, ff - cut)
    k_own = y * 2 + zh
    wait_turned = copy_or_stay(N_SEM, cot_in, turned, turn_dev, turns)
    m_up = copy(mod_in, mods.at[3], x_up)
    m_down = copy(mod_in, mods.at[1], x_down)
    m_opp = copy(mod_in, mods.at[2], x_opp)

    def spread_first(h):
        return copy(h.at[0, lo], h.at[3, lo], x_up), copy(h.at[0, hi], h.at[1, hi], x_down)

    def spread_last(h):
        return copy(h.at[0, hi], h.at[3, hi], x_up), copy(h.at[0, lo], h.at[1, lo], x_down)

    def pass_on(h, up_first, down_first):
        up_first.wait_recv()
        down_first.wait_recv()
        return copy(h.at[3, lo], h.at[2, lo], x_up), copy(h.at[1, hi], h.at[2, hi], x_down)

    h_up, h_down = spread_first(hr)
    w_far = []

    def send_w(modality, src, where):
        w_far.append(copy(src.at[where], wrt.at[1, modality, where], zl_flip))

    def flip(r, modality):
        for first in range(0, ff, 128):
            count = min(128, ff - first)
            block = wrt[r, modality, pl.ds(first, count), :]
            wr[r, modality, :, pl.ds(first, count)] = block.T

    send_w(0, wref_t_in, pl.ds(0, ff))
    for here in pol_here:
        here.wait()
    hidden(2, hp)
    for here in own:
        here.wait()
    flip(0, 0)
    flip(0, 1)

    wait_turned()
    wait_moved = copy_or_stay(N_SEM + 2, turned, cr.at[c, k_own], shift_dev, shifts)
    h_up2, h_down2 = spread_last(hr)
    h_opp_lo, h_opp_hi = pass_on(hr, h_up, h_down)
    p_up, p_down = spread_first(hp)
    p_up2, p_down2 = spread_last(hp)
    wait_moved()
    cot_zh = [copy(cr.at[c, k_own], cr.at[c, k_own], zh_flip)]
    send_w(1, wref_i_in, lo)
    send_w(1, wref_i_in, hi)
    wp_far = [
        copy(wpol_t_in, wp.at[1, :, pl.ds(0, depth)], zl_flip),
        copy(wpol_i_in, wp.at[1, :, pl.ds(depth, depth)], zl_flip),
    ]
    for got in cot_zh:
        got.wait_recv()
    pair = cr.at[c, pl.ds(y * 2, 2)]
    cot_up = copy(pair, pair, y_up)
    cot_down = copy(pair, pair, y_down)
    cot_c = [copy(pair, pair, c_flip)]
    m_up.wait_recv()
    m_down.wait_recv()
    m_opp.wait_recv()
    h_up2.wait_recv()
    h_down2.wait_recv()

    def image(d, row, where):
        return mods[d, pl.ds(row, 1), where].astype(bf16)

    def ref_piece(d, slot):
        def tile(n):
            where = lanes(n)
            img = image(d, 0, where)
            block = hr[d, :, where]
            hs[0] = block * (1 - img)
            hs[1] = block * img
            for r in range(2):
                there = pl.ds(pl.multiple_of((1 - c) * cols, cols), cols)
                away = jnp.dot(wr[r, 0, there], hs[0], preferred_element_type=f32)
                away += jnp.dot(wr[r, 1, there], hs[1], preferred_element_type=f32)
                aw[d, r, :, where] = away.astype(bf16)
                stay = pl.ds(pl.multiple_of(c * cols, cols), cols)
                kept = jnp.dot(wr[r, 0, stay], hs[0], preferred_element_type=f32)
                kept += jnp.dot(wr[r, 1, stay], hs[1], preferred_element_type=f32)
                kp[slot, r, :, where] = kept

        loop(tiles, tile)
        return copy(aw.at[d], ar.at[d], c_flip)

    def ref_sum(d, slot, got):
        got.wait_recv()

        def tile(n):
            where = lanes(n)
            for r in range(2):
                total = kp[slot, r, :, where] + ar[d, r, :, where].astype(f32)
                sr[r * 4 + d, :, where] = total.astype(bf16)

        loop(tiles, tile)

    w_far[0].wait_recv()
    flip(1, 0)
    w_far[1].wait_recv()
    w_far[2].wait_recv()
    flip(1, 1)
    got0 = ref_piece(0, 0)
    p_opp_lo, p_opp_hi = pass_on(hp, p_up, p_down)
    got1 = ref_piece(1, 1)
    ref_sum(0, 0, got0)
    got3 = ref_piece(3, 0)
    ref_sum(1, 1, got1)
    cot_up.wait_recv()
    cot_down.wait_recv()
    cot_opp_lo = copy(cr.at[c, below * 2], cr.at[c, below * 2], y_up)
    cot_opp_hi = copy(cr.at[c, above * 2 + 1], cr.at[c, above * 2 + 1], y_down)
    for at in (below, above):
        other = cr.at[c, pl.ds(at * 2, 2)]
        cot_c.append(copy(other, other, c_flip))
    h_opp_lo.wait_recv()
    h_opp_hi.wait_recv()
    got2 = ref_piece(2, 1)
    ref_sum(3, 0, got3)
    ref_sum(2, 1, got2)

    via_up = copy(sr.at[opp * 2], va, y_up)
    via_down = copy(sr.at[opp * 2 + 1], vb, y_down)
    first_up = copy(sr.at[above * 2 + 1], ga.at[1], y_up)
    first_down = copy(sr.at[below * 2], gb.at[0], y_down)

    cot_opp_lo.wait_recv()
    cot_opp_hi.wait_recv()
    other = cr.at[c, pl.ds(opp * 2, 2)]
    cot_c.append(copy(other, other, c_flip))

    def d_piece(d, store):
        def tile(n):
            where = lanes(n)
            img = image(d, 1, where)
            for r in range(2):
                for core in range(2):
                    block = cr[core, r * 4 + d, :, where]
                    at = r * 4 * cols + core * cols
                    cs[pl.ds(at, cols)] = block * (1 - img)
                    cs[pl.ds(at + 2 * cols, cols)] = block * img
            part = jnp.dot(wp[0], cs[pl.ds(0, 4 * cols)], preferred_element_type=f32)
            part += jnp.dot(wp[1], cs[pl.ds(4 * cols, 4 * cols)], preferred_element_type=f32)
            store(where, part)

        loop(tiles, tile)

    def store_dh(slot):
        def store(where, part):
            dh[slot, :, where] = part.astype(bf16)

        return store

    def down(r, core, modality):
        total = None
        for d in range(4):
            img = image(d, 1, slice(None))
            block = cr[core, r * 4 + d] * (img if modality else 1 - img)
            part = lax.dot_general(
                hp[d], block, (((1,), (1,)), ((), ())), preferred_element_type=f32
            )
            total = part if total is None else total + part
        return total

    def away(modality):
        def column(core):
            dws[modality, :, lanes(core)] = down(1, core, modality).astype(bf16)

        loop(2, column)

    for got in cot_c:
        got.wait_recv()
    p_up2.wait_recv()
    p_down2.wait_recv()
    p_opp_lo.wait_recv()
    p_opp_hi.wait_recv()
    away(0)
    dw_sent = [copy(dws.at[0], far_t, zl_flip)]
    for got in wp_far:
        got.wait_recv()
    d_piece(2, store_dh(2))
    d_via_up = copy(dh.at[2, lo], xa_via, x_up)
    d_via_down = copy(dh.at[2, hi], xb_via, x_down)
    via_up.wait_recv()
    via_down.wait_recv()

    def add_via(n):
        where = lanes(n)
        for at, via in ((above * 2, va), (below * 2 + 1, vb)):
            total = sr[at, :, where].astype(f32) + via[:, where].astype(f32)
            sr[at, :, where] = total.astype(bf16)

    loop(tiles, add_via)
    last_up = copy(sr.at[above * 2], ga.at[0], y_up)
    last_down = copy(sr.at[below * 2 + 1], gb.at[1], y_down)

    d_piece(1, store_dh(0))
    d_first_up = copy(dh.at[0, hi], xa.at[hi], x_up)
    d_piece(3, store_dh(1))
    d_first_down = copy(dh.at[1, lo], xb.at[lo], x_down)

    first_up.wait_recv()
    first_down.wait_recv()
    last_up.wait_recv()
    last_down.wait_recv()

    def y_sum(k, where):
        total = sr[y * 2 + k, :, where].astype(f32) + ga[k, :, where].astype(f32)
        return total + gb[k, :, where].astype(f32)

    def z_away(n):
        where = lanes(n)
        za[:, where] = y_sum(1 - zh, where).astype(bf16)

    loop(tiles, z_away)
    z_copy = [copy(za, zr, zh_flip)]
    away(1)

    d_via_up.wait_recv()
    d_via_down.wait_recv()

    def add_d(n):
        where = lanes(n)
        dh[0, lo, where] = (dh[0, lo, where].astype(f32) + xa_via[:, where].astype(f32)).astype(bf16)
        dh[1, hi, where] = (dh[1, hi, where].astype(f32) + xb_via[:, where].astype(f32)).astype(bf16)

    loop(tiles, add_d)
    d_last_up = copy(dh.at[0, lo], xa.at[lo], x_up)
    d_last_down = copy(dh.at[1, hi], xb.at[hi], x_down)
    dw_sent.append(copy(dws.at[1], far_i, zl_flip))

    def store_own(where, part):
        d_own[:, where] = part


    d_piece(0, store_own)
    for got in z_copy:
        got.wait_recv()

    def z_sum(n):
        where = lanes(n)
        fo[where, :] = (y_sum(zh, where) + zr[:, where].astype(f32)).T.astype(bf16)

    loop(tiles, z_sum)
    wait_back = copy_or_stay(N_SEM + 1, fo, landed, back_dev, moves)

    flushed = []
    for modality, out in enumerate((own_t, own_i)):

        def column(core, modality=modality):
            dwo[modality, :, lanes(core)] = down(0, core, modality)

        loop(2, column)
        flushed.append(local(11 + modality, dwo.at[modality], out))

    for got in (d_first_up, d_first_down, d_last_up, d_last_down):
        got.wait_recv()

    def d_sum(n):
        where = pl.ds(pl.multiple_of(n * 16, 16), 16)
        gate, up = gates[2, where].astype(f32), gates[3, where].astype(f32)
        d_hidden = d_own[where] + xa[where].astype(f32) + xb[where].astype(f32)
        sig = jax.nn.sigmoid(gate)
        gates[0, where] = (d_hidden * up * sig * (1.0 + gate * (1.0 - sig))).astype(bf16)
        gates[1, where] = (d_hidden * (gate * sig)).astype(bf16)

    loop(ff // 16, d_sum)
    flushed.append(local(13, gates.at[0], out_gate))
    flushed.append(local(14, gates.at[1], out_up))
    wait_back()

    def add_residual(n):
        where = lanes(n)
        total = landed[where, :].astype(f32) + residual[where, :].astype(f32)
        residual[where, :] = total.astype(bf16)

    loop(tiles, add_residual)
    flushed.append(local(18, residual, out_ref))
    for got in dw_sent:
        got.wait_recv()
    for here in flushed:
        here.wait()
    for rdma in started:
        rdma.wait_send()


def communicate(cot, resid, ref_mod, pol_mod, segment, margin, gate_r, up_r, gate_p, up_p, wref_t, wref_i, wpol_t, wpol_i):
    ff, rows = gate_r.shape
    cols = cot.shape[1]
    depth = wref_t.shape[1]
    cut = (ff // 32) * 16
    vmem = pltpu.VMEM
    scratch = [
        vmem((2, ff, depth), f32),
        vmem((4, ff, rows), bf16),
        vmem((cols, rows), bf16),
        vmem((rows, cols), bf16),
        vmem((rows, cols), bf16),
        vmem((rows, cols), bf16),
        vmem((cols, rows), bf16),
        vmem((8, rows), f32),
        vmem((ff, rows), f32),
        vmem((4, ff, rows), bf16),
        vmem((4, ff, rows), bf16),
        vmem((2, 2, ff, depth), bf16),
        vmem((2, 2, depth, ff), bf16),
        vmem((2, ff, 2 * depth), bf16),
        vmem((2, 8, cols, rows), bf16),
        vmem((4, 8, rows), f32),
        vmem((2, ff, 256), bf16),
        vmem((8 * cols, 256), bf16),
        vmem((4, 2, cols, rows), bf16),
        vmem((4, 2, cols, rows), bf16),
        vmem((2, 2, cols, rows), f32),
        vmem((8, cols, rows), bf16),
        vmem((cols, rows), bf16),
        vmem((cols, rows), bf16),
        vmem((2, cols, rows), bf16),
        vmem((2, cols, rows), bf16),
        vmem((cols, rows), bf16),
        vmem((cols, rows), bf16),
        vmem((rows, cols), bf16),
        vmem((3, ff, rows), bf16),
        vmem((cut, rows), bf16),
        vmem((ff - cut, rows), bf16),
        vmem((ff, rows), bf16),
        vmem((ff, rows), bf16),
        vmem((2, ff, depth), bf16),
        pltpu.SemaphoreType.DMA((N_SEM + 3,)),
        pltpu.SemaphoreType.DMA((N_SEM + 3,)),
        pltpu.SemaphoreType.DMA((19,)),
    ]
    anywhere = pl.BlockSpec(memory_space=pl.ANY)
    return pl.pallas_call(
        step_kernel,
        out_shape=(
            jax.ShapeDtypeStruct((rows, cols), bf16),
            jax.ShapeDtypeStruct((ff, rows), bf16),
            jax.ShapeDtypeStruct((ff, rows), bf16),
            jax.ShapeDtypeStruct((ff, depth), f32),
            jax.ShapeDtypeStruct((ff, depth), f32),
            jax.ShapeDtypeStruct((ff, depth), bf16),
            jax.ShapeDtypeStruct((ff, depth), bf16),
        ),
        in_specs=[anywhere] * 2 + [pl.BlockSpec(memory_space=vmem)] * 3 + [pl.BlockSpec(memory_space=pltpu.SMEM)] + [anywhere] * 8,
        out_specs=(anywhere,) * 7,
        scratch_shapes=scratch,
        compiler_params=pltpu.CompilerParams(
            collective_id=0, has_side_effects=True, vmem_limit_bytes=66_000_000
        ),
    )(cot, resid, ref_mod, pol_mod, segment, margin, gate_r, up_r, gate_p, up_p, wref_t, wref_i, wpol_t, wpol_i)


def per_device(
    ref_gate,
    ref_up,
    ref_residual,
    ref_modality,
    ref_down_text,
    ref_down_image,
    pol_gate,
    pol_up,
    pol_modality,
    pol_segment,
    pair_margin,
    token_cotangent,
    pol_down_text,
    pol_down_image,
):
    rows = ref_gate.shape[0]
    ref_out, grad_gate, grad_up, own_t, own_i, far_t, far_i = communicate(
        token_cotangent,
        ref_residual,
        ref_modality,
        pol_modality,
        pol_segment,
        pair_margin,
        ref_gate.T,
        ref_up.T,
        pol_gate.T,
        pol_up.T,
        ref_down_text.T,
        ref_down_image.T,
        pol_down_text.T,
        pol_down_image.T,
    )
    grad_t = own_t + far_t.astype(f32)
    grad_i = own_i + far_i.astype(f32)
    return (ref_out, grad_gate.T, grad_up.T, grad_t.T, grad_i.T)


def solution(mesh):
    spec = P("fsdp", "tp")
    in_specs = (
        spec,
        spec,
        spec,
        P("fsdp"),
        spec,
        spec,
        spec,
        spec,
        P("fsdp"),
        P("fsdp"),
        P(),
        spec,
        spec,
        spec,
    )
    return jax.shard_map(
        per_device, mesh=mesh, in_specs=in_specs, out_specs=(spec,) * 5, check_vma=False
    )
```
